32 devices in a mesh: gx: 4 (over y, x), gy: 8 (over z, core).
Axes of the slice: x: 2, y: 2, z: 4, core: 2. Of those that a mesh axis runs over, the one named last changes fastest.
Arguments:
- u_wind: float32 [60, 256, 1024], P(None, 'gx', 'gy'), may hold values from -6 to 6
- v_wind: float32 [60, 256, 1024], P(None, 'gx', 'gy'), may hold values from -6 to 6
- w_wind: float32 [60, 256, 1024], P(None, 'gx', 'gy'), may hold values from -3 to 3
- pressure: float32 [60, 256, 1024], P(None, 'gx', 'gy'), may hold values from -6 to 6
- vert_coef: float32 [256, 1024], P('gx', 'gy'), may hold values from 0.2 to 5
- we_slab: float32 [2, 3, 60, 5, 1024], P(None, None, None, None, ('gy', 'gx')), may hold values from -8 to 8
- sn_slab: float32 [2, 3, 60, 5, 256], P(None, None, None, None, ('gx', 'gy')), may hold values from -8 to 8
- relax_width: int32 [256, 1024], P('gx', 'gy'), may hold values from 2 to 5
Outputs:
- u_out: float32 [60, 256, 1024], P(None, 'gx', 'gy')
- v_out: float32 [60, 256, 1024], P(None, 'gx', 'gy')
- w_out: float32 [60, 256, 1024], P(None, 'gx', 'gy')
- p_out: float32 [60, 256, 1024], P(None, 'gx', 'gy')
The draws below stay inside these ranges and needn't reach their ends.
All inputs are finite; a program needn't handle non-finite values.
Results may differ from the reference program's by a relative error of at most 0.0001.
Values sent between devices are 32-bit elements; how exact they have to be, the bound alone decides.
No kernel may reach another device: no remote copies, remote signals or barrier semaphores. Data moves between devices by JAX's collectives and lax.ppermute only.
A program may use at most 192 MiB of HBM per device.

```python
import math
import jax
import jax.numpy as jnp
from jax import lax

NZ = 60
W = 5
SUBSTEPS = 6
NX = 256
NY = 1024


def place_ends(drawn, stream_key, smallest, largest):
    shape = drawn.shape
    place = [jax.random.randint(jax.random.fold_in(stream_key, axis), (), 0, shape[axis]) for axis in range(len(shape))]
    drawn = drawn.at[tuple(place)].set(smallest)
    longest = shape.index(max(shape))
    place[longest] = (place[longest] + 1) % shape[longest]
    return drawn.at[tuple(place)].set(largest)


def level_of(rng, shape, split, smallest, high):
    level = 1.0
    for position, blocks in split:
        draws = jax.random.uniform(jax.random.fold_in(jax.random.fold_in(rng, 6), position), (blocks,), jnp.float32, smallest / len(split), high / len(split))
        level = level * jnp.repeat(jnp.exp(draws), shape[position] // blocks).reshape((-1,) + (1,) * (len(shape) - 1 - position))
    return level


def normal_values(own_key, dims, deviation, bound, pieces=(), kind=jnp.bfloat16):
    array = deviation * jax.random.normal(own_key, dims, jnp.float32)
    if pieces:
        array = array * level_of(own_key, dims, pieces, -0.22, 0.18)
    return jnp.clip(array, -bound, bound).astype(kind)


def setup_inputs(seed: int = 0) -> dict:
    seeds = jax.random.split(jax.random.key(seed), 9)
    u_wind = normal_values(seeds[0], (NZ, NX, NY), 1.0, 6.0, ((1, 4), (2, 8)), jnp.float32)
    v_wind = normal_values(seeds[1], (NZ, NX, NY), 1.0, 6.0, ((1, 4), (2, 8)), jnp.float32)
    w_wind = normal_values(seeds[2], (NZ, NX, NY), 0.5, 3.0, ((1, 4), (2, 8)), jnp.float32)
    pressure = normal_values(seeds[3], (NZ, NX, NY), 1.0, 6.0, ((1, 4), (2, 8)), jnp.float32)
    vert_coef = jnp.clip(jnp.exp(math.log(5.0) - 3.218876 * jax.random.uniform(seeds[4], (NX, NY), jnp.float32) ** level_of(seeds[4], (NX, NY), ((0, 4), (1, 8)), -0.2, 0.2)), 0.2, 5.0)
    we_slab = normal_values(seeds[5], (2, 3, NZ, W, NY), 1.5, 8.0, ((4, 32),), jnp.float32)
    sn_slab = normal_values(seeds[6], (2, 3, NZ, W, NX), 1.5, 8.0, ((4, 32),), jnp.float32)
    relax_width = place_ends(jax.random.randint(seeds[7], (NX, NY), 2, W + 1), jax.random.fold_in(seeds[7], 1), 2, W).astype(jnp.int32)
    return dict(u_wind=u_wind, v_wind=v_wind, w_wind=w_wind, pressure=pressure, vert_coef=vert_coef, we_slab=we_slab, sn_slab=sn_slab, relax_width=relax_width)


accel = 0.3
spread = 0.3
buoyancy = 0.5


def tri_solve(coef, rhs):
    def forward(carry, item):
        prev_c, prev_d = carry
        denom = 1.0 + 2.0 * coef + coef * prev_c
        next_c = -coef / denom
        next_d = (item + coef * prev_d) / denom
        return (next_c, next_d), (next_c, next_d)

    zero = jnp.zeros_like(coef)
    _, (cees, dees) = lax.scan(forward, (zero, zero), rhs)

    def backward(above, item):
        c_here, d_here = item
        value = d_here - c_here * above
        return value, value

    _, solved = lax.scan(backward, zero, (cees, dees), reverse=True)
    return solved


def blend(field, rows_k, cols_k, xpos, ypos, nx_total, ny_total, rate):
    band = rows_k.shape[2]
    size_x = field.shape[1]
    size_y = field.shape[2]
    west = jnp.pad(rows_k[0], ((0, 0), (0, size_x - band), (0, 0)))
    east = jnp.pad(rows_k[1][:, ::-1, :], ((0, 0), (size_x - band, 0), (0, 0)))
    south = jnp.pad(jnp.transpose(cols_k[0], (0, 2, 1)), ((0, 0), (0, 0), (0, size_y - band)))
    north = jnp.pad(jnp.transpose(cols_k[1][:, ::-1, :], (0, 2, 1)), ((0, 0), (0, 0), (size_y - band, 0)))
    weight_w = jnp.maximum(rate - xpos[:, None], 0.0) / rate
    weight_e = jnp.maximum(rate - (nx_total - 1.0 - xpos)[:, None], 0.0) / rate
    weight_s = jnp.maximum(rate - ypos[None, :], 0.0) / rate
    weight_n = jnp.maximum(rate - (ny_total - 1.0 - ypos)[None, :], 0.0) / rate
    field = field + weight_w[None] * (west - field)
    field = field + weight_e[None] * (east - field)
    field = field + weight_s[None] * (south - field)
    field = field + weight_n[None] * (north - field)
    return field


def column_part(u_new, v_new, west_u, south_v, w_old, p_old, coef):
    diverge = (u_new - west_u) + (v_new - south_v)
    sectioned = p_old - spread * diverge
    above_q = jnp.concatenate([sectioned[1:], jnp.zeros_like(sectioned[:1])], axis=0)
    rhs = w_old + buoyancy * (sectioned - above_q)
    w_new = tri_solve(coef, rhs)
    below_w = jnp.concatenate([jnp.zeros_like(w_new[:1]), w_new[:-1]], axis=0)
    p_new = sectioned - buoyancy * (w_new - below_w)
    return w_new, p_new


def reference(u_wind, v_wind, w_wind, pressure, vert_coef, we_slab, sn_slab, relax_width):
    size_x = pressure.shape[1]
    size_y = pressure.shape[2]
    xpos = jnp.arange(size_x, dtype=jnp.int32).astype(jnp.float32)
    ypos = jnp.arange(size_y, dtype=jnp.int32).astype(jnp.float32)
    rate = relax_width.astype(jnp.float32)
    fields = []
    for index, field in enumerate((u_wind, v_wind, pressure)):
        fields.append(blend(field, we_slab[:, index], sn_slab[:, index], xpos, ypos, float(size_x), float(size_y), rate))
    u_now, v_now, p_now = fields
    w_now = w_wind
    for step in range(SUBSTEPS):
        east_p = jnp.concatenate([p_now[:, 1:, :], jnp.zeros_like(p_now[:, :1, :])], axis=1)
        north_p = jnp.concatenate([p_now[:, :, 1:], jnp.zeros_like(p_now[:, :, :1])], axis=2)
        u_now = u_now - accel * (east_p - p_now)
        v_now = v_now - accel * (north_p - p_now)
        west_u = jnp.concatenate([jnp.zeros_like(u_now[:, :1, :]), u_now[:, :-1, :]], axis=1)
        south_v = jnp.concatenate([jnp.zeros_like(v_now[:, :, :1]), v_now[:, :, :-1]], axis=2)
        w_now, p_now = column_part(u_now, v_now, west_u, south_v, w_now, p_now, vert_coef)
    return u_now, v_now, w_now, p_now
```

```python
import functools
import jax
import jax.numpy as jnp
from jax import lax
from jax.experimental import pallas as pl
from jax.experimental.pallas import tpu as pltpu
from jax.sharding import PartitionSpec as P

SUBSTEPS = 6
ACCEL = 0.3
SPREAD = 0.3
BUOYANCY = 0.5
DEEP = 6
GROUP = 2 * DEEP
ZC = 20
SUBL = 8
LANES = 128
F32 = jnp.float32


def lane_ids():
    return lax.broadcasted_iota(jnp.int32, (SUBL, LANES), 1)


def sub_ids():
    return lax.broadcasted_iota(jnp.int32, (SUBL, LANES), 0)


def lroll(x, shift):
    if isinstance(shift, int):
        shift = shift % LANES
        if shift == 0:
            return x
    return pltpu.roll(x, shift, 1)


def sroll(x, shift):
    return pltpu.roll(x, shift % SUBL, 0)


def pack_slabs(we, sn, west, east, south, north):
    band, m = we.shape[3], we.shape[4]
    xs = sn.shape[3]
    west[...] = jnp.zeros_like(west)
    east[...] = jnp.zeros_like(east)
    south[...] = jnp.zeros_like(south)
    north[...] = jnp.zeros_like(north)
    for f in range(3):
        for z in range(ZC):
            g, c = divmod(z, 4)
            west[0, f, g, 0:band, m * c : m * (c + 1)] = we[0, f, z]
            east[0, f, g, 0:band, m * c : m * (c + 1)] = we[1, f, z]
            t, c = divmod(z, 10)
            lo = GROUP * c
            s_val = sn[0, f, z]
            n_val = sn[1, f, z]
            for rep in range(SUBL // xs):
                rows = slice(xs * rep, xs * (rep + 1))
                south[0, f, t, rows, lo : lo + band] = s_val
                for d in range(band):
                    at = lo + band - 1 - d
                    north[0, f, t, rows, at : at + 1] = n_val[:, d : d + 1]


def blend_pack(n_gx, n_gy, m, xs, band, *refs):
    u, v, p, w, r, rate = refs[:6]
    refs = refs[6:]
    we_own = refs[:2]
    sn_own = refs[2:4]
    we_in = refs[4 : 4 + n_gx - 1]
    sn_in = refs[3 + n_gx : 3 + n_gx + n_gy - 1]
    ub, vb, pb, xa, xb, q, c_out = refs[2 + n_gx + n_gy :]
    gx = lax.axis_index("gx")
    gy = lax.axis_index("gy")
    size_x = u.shape[1]
    blocks = size_x // SUBL
    outs = (ub, vb, pb)
    for src, dst in zip((u, v, p), outs):
        dst[...] = src[...]
    lane = lane_ids()
    sub = sub_ids()

    def band_rows(pieces, f, z):
        g, c = z // 4, z % 4
        val = jnp.zeros((SUBL, LANES), F32)
        for s, piece in enumerate(pieces):
            moved = pltpu.roll(piece[0, f, g], jnp.mod(m * s - m * c, LANES), 1)
            val = jnp.where((lane >= m * s) & (lane < m * (s + 1)), moved, val)
        return val

    @pl.when(gx == 0)
    def _():
        pieces = [we_own[0]] + [we_in[s - 1] for s in range(1, n_gx)]
        rt = rate[0:SUBL, :].astype(F32)
        wt = jnp.maximum(rt - sub.astype(F32), 0.0) / rt

        def body(z, carry):
            for f in range(3):
                val = band_rows(pieces, f, z)
                old = outs[f][z, 0:SUBL, :]
                outs[f][z, 0:SUBL, :] = old + wt * (val - old)
            return carry

        lax.fori_loop(0, ZC, body, 0)

    @pl.when(gx == n_gx - 1)
    def _():
        pieces = [we_in[n_gx - 2 - s] for s in range(n_gx - 1)] + [we_own[1]]
        rt = rate[size_x - SUBL : size_x, :].astype(F32)
        wt = jnp.maximum(rt - (SUBL - 1 - sub).astype(F32), 0.0) / rt

        def body(z, carry):
            for f in range(3):
                val = band_rows(pieces, f, z)
                turned = sroll(val, 1)
                turned = jnp.where(sub % 4 == 1, sroll(val, 3), turned)
                turned = jnp.where(sub % 4 == 2, sroll(val, 5), turned)
                turned = jnp.where(sub % 4 == 3, sroll(val, 7), turned)
                old = outs[f][z, size_x - SUBL : size_x, :]
                outs[f][z, size_x - SUBL : size_x, :] = old + wt * (turned - old)
            return carry

        lax.fori_loop(0, ZC, body, 0)

    per = SUBL // xs

    def side_blend(pieces, first, dist):
        wts = []
        for b in range(blocks):
            rt = rate[SUBL * b : SUBL * (b + 1), :].astype(F32)
            wts.append(jnp.maximum(rt - dist, 0.0) / rt)

        def body(z, carry):
            t, c = z // 10, z % 10
            shift = jnp.mod(first - GROUP * c + LANES, LANES)
            for f in range(3):
                for b in range(blocks):
                    val = pieces[b * per][0, f, t]
                    for s in range(1, per):
                        val = jnp.where(sub // xs == s, pieces[b * per + s][0, f, t], val)
                    val = pltpu.roll(val, shift, 1)
                    old = outs[f][z, SUBL * b : SUBL * (b + 1), :]
                    outs[f][z, SUBL * b : SUBL * (b + 1), :] = old + wts[b] * (val - old)
            return carry

        lax.fori_loop(0, ZC, body, 0)

    @pl.when(gy == 0)
    def _():
        pieces = [sn_own[0]] + [sn_in[s - 1] for s in range(1, n_gy)]
        side_blend(pieces, 0, lane.astype(F32))

    @pl.when(gy == n_gy - 1)
    def _():
        pieces = [sn_in[n_gy - 2 - s] for s in range(n_gy - 1)] + [sn_own[1]]
        side_blend(pieces, LANES - band, (LANES - 1 - lane).astype(F32))

    even = (gx % 2) == 0
    top = size_x - SUBL

    def strip_of(blocks_of):
        acc = jnp.zeros((SUBL, LANES), F32)
        for b in range(blocks):
            lo = GROUP * (b + 1)
            moved = lroll(blocks_of(b), lo + DEEP)
            acc = jnp.where((lane >= lo) & (lane < lo + GROUP), moved, acc)
        return acc

    def corner_of(strip, spot, acc):
        o = 2 * GROUP * spot
        acc = jnp.where((lane >= o) & (lane < o + GROUP), lroll(strip, o - GROUP * blocks), acc)
        return jnp.where(
            (lane >= o + GROUP) & (lane < o + 2 * GROUP), lroll(strip, o), acc
        )

    def body(h, carry):
        corners = [jnp.zeros((SUBL, LANES), F32)] * 4
        for c5 in range(5):
            z = h * 5 + c5
            for f, src in enumerate((ub, vb, pb, w)):
                strip = strip_of(lambda b: src[z, SUBL * b : SUBL * (b + 1), :])
                q[0, f * ZC + z] = strip
                corners[f] = corner_of(strip, c5, corners[f])
            u7 = ub[z, top:, :]
            u0 = ub[z, 0:SUBL, :]
            v7 = vb[z, top:, :]
            v0 = vb[z, 0:SUBL, :]
            up7 = ub[z, top - 1 : size_x - 1, :]
            up0 = jnp.where(sub == 0, 0.0, sroll(u0, 1))
            e7 = SPREAD * ((u7 - up7) + (v7 - jnp.where(lane == 0, 0.0, lroll(v7, 1))))
            e0 = SPREAD * ((u0 - up0) + (v0 - jnp.where(lane == 0, 0.0, lroll(v0, 1))))
            ea = jnp.where(sub < 2, sroll(e7, -3), pb[z, top:, :])
            eb = jnp.where(sub < 3, sroll(e7, -5), w[z, top:, :])
            wa = jnp.where(sub < 6, pb[z, 0:SUBL, :], sroll(e0, 6))
            wb = jnp.where(sub < 5, w[z, 0:SUBL, :], sroll(e0, 3))
            at = 2 * SUBL * c5
            xa[h, at : at + SUBL, :] = jnp.where(even, ea, wa)
            xa[h, at + SUBL : at + 2 * SUBL, :] = jnp.where(even, eb, wb)
            xb[h, at : at + SUBL, :] = jnp.where(even, wa, ea)
            xb[h, at + SUBL : at + 2 * SUBL, :] = jnp.where(even, wb, eb)
            last = ub[z, size_x - 1 : size_x, :]
            xa[h, 80 + c5 : 81 + c5, :] = last
            xb[h, 80 + c5 : 81 + c5, :] = last
        for f in range(4):
            c_out[0, f * (ZC // 5) + h] = corners[f]
        return carry

    lax.fori_loop(0, ZC // 5, body, 0)
    strip = strip_of(lambda b: r[SUBL * b : SUBL * (b + 1), :])
    q[0, 4 * ZC] = strip
    c_out[0, 4 * (ZC // 5)] = corner_of(strip, 0, jnp.zeros((SUBL, LANES), F32))
    east_r = r[size_x - 5 : size_x, :]
    west_r = r[0:5, :]
    ra = jnp.where(even, east_r, west_r)
    rb = jnp.where(even, west_r, east_r)
    for ref, val in ((xa, ra), (xb, rb)):
        ref[0, 85:88, :] = val[0:3]
        ref[1, 85:87, :] = val[3:5]
        ref[1, 87:88, :] = val[4:5]
        ref[2, 85:88, :] = val[0:3]
        ref[3, 85:88, :] = val[0:3]


def substeps(n_gx, n_gy, *refs):
    (ub, vb, pb, w, r, xa, xb, qa, qb, ca, cb, caa, cab, cba, cbb) = refs[:15]
    (u_out, v_out, w_out, p_out) = refs[15:19]
    (PM, EM, WM, GM, QM, SM, PS, ES, WS, GS, QS, SS, RM) = refs[19:]
    levels, size_x = ub.shape[0], ub.shape[1]
    blocks = size_x // SUBL
    full = blocks + 2
    gx = lax.axis_index("gx")
    gy = lax.axis_index("gy")
    x_even = (gx % 2) == 0
    y_even = (gy % 2) == 0
    is_w, is_e = gx == 0, gx == n_gx - 1
    is_s, is_n = gy == 0, gy == n_gy - 1
    lane = lane_ids()
    sub = sub_ids()
    within = lane % GROUP
    block_of = lane // GROUP
    low_half = within < DEEP
    own_rows = (block_of >= 1) & (block_of <= blocks)
    zero = jnp.zeros((SUBL, LANES), F32)

    def strip_from(qs, qn, cw, ce, spot):
        o = 2 * GROUP * spot
        mine = jnp.where(low_half, qs, qn)
        got = jnp.where(block_of == 0, pltpu.roll(cw, jnp.mod(LANES - o, LANES), 1), mine)
        return jnp.where(
            block_of == full - 1,
            pltpu.roll(ce, jnp.mod(LANES + GROUP * blocks - o, LANES), 1),
            got,
        )

    def four(k, i):
        aa, ab, ba, bb = caa[k, i], cab[k, i], cba[k, i], cbb[k, i]
        xa_ya = jnp.where(y_even, ab, aa)
        xa_yb = jnp.where(y_even, aa, ab)
        xb_ya = jnp.where(y_even, bb, ba)
        xb_yb = jnp.where(y_even, ba, bb)
        sw = jnp.where(x_even, xb_ya, xa_ya)
        nw = jnp.where(x_even, xb_yb, xa_yb)
        se = jnp.where(x_even, xa_ya, xb_ya)
        ne = jnp.where(x_even, xa_yb, xb_yb)
        return jnp.where(low_half, sw, nw), jnp.where(low_half, se, ne)

    def strip_at(k, iq, ic, spot):
        a, b = qa[k, iq], qb[k, iq]
        cw, ce = four(k, ic)
        return strip_from(jnp.where(y_even, b, a), jnp.where(y_even, a, b), cw, ce, spot)

    def xneigh(s):
        up = sroll(s, 1)
        up = jnp.where(sub == 0, lroll(up, GROUP), up)
        dn = sroll(s, -1)
        dn = jnp.where(sub == SUBL - 1, lroll(dn, -GROUP), dn)
        return up, dn

    def edge_pack(tiles):
        acc = zero
        for b, tile in tiles:
            lo = GROUP * b + DEEP
            acc = jnp.where((lane == lo) | (lane == lo - 1), lroll(tile, lo), acc)
        return acc

    rims = ((within == DEEP - 1), (within == DEEP))

    def fix_main(tiles):
        first = jnp.where(is_w & (sub == SUBL - 1), sroll(tiles[1], -1), tiles[0])
        last = jnp.where(is_e & (sub == 0), 0.0, tiles[full - 1])
        return [first] + tiles[1:-1] + [last]

    def fix_strip_x(s):
        _, dn = xneigh(s)
        s = jnp.where(is_w & (block_of == 0) & (sub == SUBL - 1), dn, s)
        return jnp.where(is_e & (block_of == full - 1) & (sub == 0), 0.0, s)

    for b in range(blocks):
        RM[SUBL * (b + 1) : SUBL * (b + 2), :] = r[SUBL * b : SUBL * (b + 1), :]
    west_x = lambda h, lo, hi: jnp.where(x_even, xb[h, lo:hi, :], xa[h, lo:hi, :])
    east_x = lambda h, lo, hi: jnp.where(x_even, xa[h, lo:hi, :], xb[h, lo:hi, :])
    RM[0:SUBL, :] = jnp.ones((SUBL, LANES), F32)
    RM[SUBL * (full - 1) : SUBL * full, :] = jnp.ones((SUBL, LANES), F32)
    RM[3:6, :] = west_x(0, 85, 88)
    RM[6:8, :] = west_x(1, 85, 87)
    lo = SUBL * (full - 1)
    RM[lo : lo + 3, :] = east_x(0, 85, 88)
    RM[lo + 3 : lo + 5, :] = east_x(1, 85, 87)
    coefs = [RM[SUBL * b : SUBL * (b + 1), :] for b in range(full)]
    coefs.append(strip_at(0, 4 * ZC, 4 * (ZC // 5), 0))
    coefs = [jnp.where(c > 0.0, c, 1.0) for c in coefs]
    RM[SUBL * full :, :] = coefs[-1]
    for b in range(full):
        RM[SUBL * b : SUBL * (b + 1), :] = coefs[b]
    kappas = [2.0 * c / ((1.0 + 2.0 * c) + jnp.sqrt(1.0 + 4.0 * c)) for c in coefs]
    rhos = [k * k for k in kappas]

    def factor_body(z, carry):
        powers, lows = carry
        new_p, new_l = [], []
        for b in range(full + 1):
            nxt = powers[b] * rhos[b]
            high = 1.0 - nxt
            g = kappas[b] * (lows[b] / high)
            if b < full:
                GM[z, SUBL * b : SUBL * (b + 1), :] = g
            else:
                GS[z] = g
            new_p.append(nxt)
            new_l.append(high)
        return tuple(new_p), tuple(new_l)

    lax.fori_loop(
        0, levels, factor_body, (tuple(rhos), tuple(1.0 - x for x in rhos))
    )

    def unpack(z, carry):
        k, zz = z // ZC, z % ZC
        h, c5 = z // 5, z % 5
        s5 = ZC // 5
        hh = zz // 5
        strips = []
        for f in range(4):
            strips.append(strip_at(k, f * ZC + zz, f * s5 + hh, c5))
        us, vs, ps, ws = strips
        at = pl.multiple_of(2 * SUBL * c5, SUBL)
        xa_a, xa_b = xa[h, pl.ds(at, SUBL), :], xa[h, pl.ds(at + SUBL, SUBL), :]
        xb_a, xb_b = xb[h, pl.ds(at, SUBL), :], xb[h, pl.ds(at + SUBL, SUBL), :]
        wa, wb = jnp.where(x_even, xb_a, xa_a), jnp.where(x_even, xb_b, xa_b)
        ea, eb = jnp.where(x_even, xa_a, xb_a), jnp.where(x_even, xa_b, xb_b)
        e_west = jnp.where(sub < 5, sroll(wa, 3), sroll(wb, 5))
        e_east = jnp.where(sub < 2, sroll(ea, 2), sroll(eb, -3))
        u_row = jnp.where(
            x_even, xb[h, pl.ds(80 + c5, 1), :], xa[h, pl.ds(80 + c5, 1), :]
        )
        u_row = jnp.where(is_w, 0.0, u_row)
        o = 2 * GROUP * c5
        i_v = s5 + hh
        cw = jnp.where(x_even, cb[k, i_v], ca[k, i_v])
        ce = jnp.where(x_even, ca[k, i_v], cb[k, i_v])
        vm = [vb[z, SUBL * b : SUBL * (b + 1), :] for b in range(blocks)]
        vpack = edge_pack([(b + 1, vm[b]) for b in range(blocks)])
        vpack = jnp.where(block_of == 0, pltpu.roll(cw, jnp.mod(LANES - o, LANES), 1), vpack)
        vpack = jnp.where(
            block_of == full - 1,
            pltpu.roll(ce, jnp.mod(LANES + GROUP * blocks - o, LANES), 1),
            vpack,
        )
        u_up, _ = xneigh(us)
        v_left = jnp.where(within == DEEP, lroll(vpack, 1), lroll(vs, 1))
        es = SPREAD * ((us - u_up) + (vs - v_left))
        ES[z] = es
        ps = fix_strip_x(ps)
        PS[z] = ps
        WS[z] = ws
        SS[z] = zero
        tiles = [wa] + [pb[z, SUBL * b : SUBL * (b + 1), :] for b in range(blocks)] + [ea]
        tiles = fix_main(tiles)
        for b in range(full):
            PM[z, SUBL * (b + 1) : SUBL * (b + 2), :] = tiles[b]
            v_rim = jnp.where(lane == 0, lroll(vs, -(GROUP * b + DEEP - 1)), 0.0)
            if b == 0:
                e = e_west - SPREAD * v_rim
                ww = wb
            elif b == full - 1:
                u63 = jnp.where(sub == 0, sroll(ub[z, size_x - SUBL :, :], 1), 0.0)
                e = e_east - SPREAD * (v_rim + u63)
                ww = eb
            else:
                m = b - 1
                uu = ub[z, SUBL * m : SUBL * (m + 1), :]
                if m == 0:
                    up = jnp.where(sub == 0, u_row, sroll(uu, 1))
                else:
                    up = ub[z, SUBL * m - 1 : SUBL * (m + 1) - 1, :]
                left = jnp.where(lane == 0, v_rim, lroll(vm[m], 1))
                e = SPREAD * ((uu - up) + (vm[m] - left))
                ww = w[z, SUBL * m : SUBL * (m + 1), :]
                SM[z, SUBL * m : SUBL * (m + 1), :] = zero
            EM[z, SUBL * b : SUBL * (b + 1), :] = e
            WM[z, SUBL * b : SUBL * (b + 1), :] = ww
        SM[z, size_x:, :] = zero
        PM[z, 0:SUBL, :] = zero
        PM[z, SUBL * (full + 1) :, :] = zero
        return carry

    lax.fori_loop(0, levels, unpack, 0)

    rinvs = lambda b: RM[SUBL * b : SUBL * (b + 1), :]
    for b in range(full + 1):
        RM[SUBL * b : SUBL * (b + 1), :] = 1.0 / RM[SUBL * b : SUBL * (b + 1), :]

    coef_step = ACCEL * SPREAD

    def step(_, carry):
        def sections(z):
            qs = []
            ps = PS[z]
            mains = [PM[z, SUBL * (b + 1) : SUBL * (b + 2), :] for b in range(full)]
            cpack = edge_pack(list(enumerate(mains)))
            ps = jnp.where(is_s & rims[0], lroll(cpack, -1), ps)
            ps = jnp.where(is_n & rims[1], 0.0, ps)
            for b in range(full):
                p0 = mains[b]
                up = PM[z, SUBL * (b + 1) - 1 : SUBL * (b + 2) - 1, :]
                dn = PM[z, SUBL * (b + 1) + 1 : SUBL * (b + 2) + 1, :]
                t = lroll(ps, -(GROUP * b + DEEP))
                lf = lroll(jnp.where(lane == LANES - 1, t, p0), 1)
                rt = lroll(jnp.where(lane == 0, t, p0), -1)
                lap = ((lf + rt) + (up + dn)) - 4.0 * p0
                e = EM[z, SUBL * b : SUBL * (b + 1), :] - coef_step * lap
                EM[z, SUBL * b : SUBL * (b + 1), :] = e
                qq = p0 - e
                QM[z, SUBL * b : SUBL * (b + 1), :] = qq
                qs.append(qq)
                if b >= 1:
                    m = b - 1
                    SM[z, SUBL * m : SUBL * (m + 1), :] += p0
            up, dn = xneigh(ps)
            lf = jnp.where(rims[1], lroll(cpack, 1), lroll(ps, 1))
            rt = jnp.where(rims[0], lroll(cpack, -1), lroll(ps, -1))
            lap = ((lf + rt) + (up + dn)) - 4.0 * ps
            e = ES[z] - coef_step * lap
            ES[z] = e
            qq = ps - e
            QS[z] = qq
            SS[z] += ps
            qs.append(qq)
            return qs

        def eliminate(z, q_here, q_next, d_prev):
            ds = []
            for b in range(full + 1):
                if b < full:
                    sl = (z, slice(SUBL * b, SUBL * (b + 1)), slice(None))
                    wv, g = WM[sl], GM[sl]
                else:
                    wv, g = WS[z], GS[z]
                rhs = wv + BUOYANCY * (q_here[b] - q_next[b])
                d = g * (rhs * rinvs(b) + d_prev[b])
                if b < full:
                    WM[sl] = d
                else:
                    WS[z] = d
                ds.append(d)
            return ds

        def forward(z, carry):
            q_prev, d_prev = carry
            q_now = sections(z)
            ds = eliminate(z - 1, q_prev, q_now, d_prev)
            return tuple(q_now), tuple(ds)

        q0 = sections(0)
        zeros = tuple([zero] * (full + 1))
        q_last, d_last = lax.fori_loop(1, levels, forward, (tuple(q0), zeros))
        ds = eliminate(levels - 1, q_last, zeros, d_last)

        def finish(z, above, here):
            tiles = []
            for b in range(full + 1):
                qv = QM[z, SUBL * b : SUBL * (b + 1), :] if b < full else QS[z]
                tiles.append(qv - BUOYANCY * (above[b] - here[b]))
            mains = fix_main(tiles[:full])
            for b in range(full):
                PM[z, SUBL * (b + 1) : SUBL * (b + 2), :] = mains[b]
            PS[z] = fix_strip_x(tiles[full])

        def backward(i, above):
            z = levels - 2 - i
            here = []
            for b in range(full + 1):
                if b < full:
                    sl = (z, slice(SUBL * b, SUBL * (b + 1)), slice(None))
                    val = WM[sl] + GM[sl] * above[b]
                    WM[sl] = val
                else:
                    val = WS[z] + GS[z] * above[b]
                    WS[z] = val
                here.append(val)
            finish(z + 1, above, here)
            return tuple(here)

        bottom = lax.fori_loop(0, levels - 1, backward, tuple(ds))
        finish(0, bottom, zeros)
        return carry

    lax.fori_loop(0, SUBSTEPS, step, 0)

    def emit(z, carry):
        ss = SS[z]
        for m in range(blocks):
            rows = slice(SUBL * m, SUBL * (m + 1))
            s0 = SM[z, rows, :]
            dn = SM[z, SUBL * m + 1 : SUBL * (m + 1) + 1, :]
            t = lroll(ss, -(GROUP * (m + 1) + DEEP))
            rt = lroll(jnp.where(lane == 0, t, s0), -1)
            u_out[z, rows, :] = ub[z, rows, :] - ACCEL * (dn - s0)
            v_out[z, rows, :] = vb[z, rows, :] - ACCEL * (rt - s0)
            w_out[z, rows, :] = WM[z, SUBL * (m + 1) : SUBL * (m + 2), :]
            p_out[z, rows, :] = PM[z, SUBL * (m + 2) : SUBL * (m + 3), :]
        return carry

    lax.fori_loop(0, levels, emit, 0)


def swap(block, axis, second):
    n = lax.axis_size(axis)
    return lax.ppermute(block, axis, pairing(n, second))


def pairing(n, second):
    lo = 1 if second else 0
    pairs = []
    for i in range(lo, n - 1, 2):
        pairs += [(i, i + 1), (i + 1, i)]
    return pairs


def swap2(block, second_x, second_y):
    nx, ny = lax.axis_size("gx"), lax.axis_size("gy")
    pairs = []
    for a, b in pairing(nx, second_x):
        for c, d in pairing(ny, second_y):
            pairs.append((a * ny + c, b * ny + d))
    return lax.ppermute(block, ("gx", "gy"), pairs)


def to_ends(low, high, axis):
    n = lax.axis_size(axis)
    me = lax.axis_index(axis)
    got = []
    for k in range(1, n):
        block = jnp.where(me == k, low, high)
        got.append(lax.ppermute(block, axis, [(k, 0), (n - 1 - k, n - 1)]))
    return got


def per_device(u_wind, v_wind, w_wind, pressure, vert_coef, we_slab, sn_slab, relax_width):
    n_gx, n_gy = lax.axis_size("gx"), lax.axis_size("gy")
    levels, size_x, size_y = pressure.shape
    blocks = size_x // SUBL
    full = blocks + 2
    band, m = we_slab.shape[3], we_slab.shape[4]
    xs = sn_slab.shape[4]
    steps = levels // ZC
    sds = jax.ShapeDtypeStruct
    big = pltpu.CompilerParams(vmem_limit_bytes=60 * 1024 * 1024)

    sn_t = jnp.transpose(sn_slab, (0, 1, 2, 4, 3))
    we_shape = (steps, 3, ZC // 4, SUBL, LANES)
    sn_shape = (steps, 3, ZC // 10, SUBL, LANES)
    lead = lambda shape: pl.BlockSpec((1,) + shape[1:], lambda i: (i,) + (0,) * (len(shape) - 1))
    west, east, south, north = pl.pallas_call(
        pack_slabs,
        grid=(steps,),
        in_specs=[
            pl.BlockSpec((2, 3, ZC, band, m), lambda i: (0, 0, i, 0, 0)),
            pl.BlockSpec((2, 3, ZC, xs, band), lambda i: (0, 0, i, 0, 0)),
        ],
        out_specs=[lead(we_shape)] * 2 + [lead(sn_shape)] * 2,
        out_shape=[sds(we_shape, F32)] * 2 + [sds(sn_shape, F32)] * 2,
        name="pack_slabs",
    )(we_slab, sn_t)
    we_in = to_ends(west, east, "gx")
    sn_in = to_ends(south, north, "gy")

    field = pl.BlockSpec((ZC, size_x, size_y), lambda i: (i, 0, 0))
    plane = pl.BlockSpec((size_x, size_y), lambda i: (0, 0))
    x_shape = (levels // 5, 88, LANES)
    q_shape = (steps, 4 * ZC + 1, SUBL, LANES)
    c_shape = (steps, 4 * (ZC // 5) + 1, SUBL, LANES)
    ub, vb, pb, xa, xb, q, c = pl.pallas_call(
        functools.partial(blend_pack, n_gx, n_gy, m, xs, band),
        grid=(steps,),
        in_specs=[field] * 4
        + [plane] * 2
        + [lead(we_shape)] * 2
        + [lead(sn_shape)] * 2
        + [lead(we_shape)] * (n_gx - 1)
        + [lead(sn_shape)] * (n_gy - 1),
        out_specs=[field] * 3
        + [pl.BlockSpec((ZC // 5, 88, LANES), lambda i: (i, 0, 0))] * 2
        + [lead(q_shape), lead(c_shape)],
        out_shape=[sds(pressure.shape, F32)] * 3
        + [sds(x_shape, F32)] * 2
        + [sds(q_shape, F32), sds(c_shape, F32)],
        compiler_params=big,
        name="blend_pack",
    )(
        u_wind, v_wind, pressure, w_wind, vert_coef, relax_width,
        west, east, south, north, *we_in, *sn_in,
    )
    xa = swap(xa, "gx", False)
    xb = swap(xb, "gx", True)
    qa = swap(q, "gy", False)
    qb = swap(q, "gy", True)
    ca = swap(c, "gx", False)
    cb = swap(c, "gx", True)
    caa = swap2(c, False, False)
    cab = swap2(c, False, True)
    cba = swap2(c, True, False)
    cbb = swap2(c, True, True)

    whole = pl.BlockSpec(memory_space=pltpu.VMEM)
    tall = pltpu.VMEM((levels, SUBL * full, LANES), F32)
    strip = pltpu.VMEM((levels, SUBL, LANES), F32)
    return pl.pallas_call(
        functools.partial(substeps, n_gx, n_gy),
        in_specs=[whole] * 15,
        out_specs=[whole] * 4,
        out_shape=[sds(pressure.shape, F32)] * 4,
        scratch_shapes=[
            pltpu.VMEM((levels, SUBL * (full + 2), LANES), F32),
            tall, tall, tall, tall,
            pltpu.VMEM((levels, SUBL * (blocks + 1), LANES), F32),
            strip, strip, strip, strip, strip, strip,
            pltpu.VMEM((SUBL * (full + 1), LANES), F32),
        ],
        compiler_params=big,
        name="substeps",
    )(ub, vb, pb, w_wind, vert_coef, xa, xb, qa, qb, ca, cb, caa, cab, cba, cbb)


def solution(mesh):
    cell = P(None, "gx", "gy")
    placed = (
        cell, cell, cell, cell,
        P("gx", "gy"),
        P(None, None, None, None, ("gy", "gx")),
        P(None, None, None, None, ("gx", "gy")),
        P("gx", "gy"),
    )
    return jax.shard_map(
        per_device,
        mesh=mesh,
        in_specs=placed,
        out_specs=(cell, cell, cell, cell),
        check_vma=False,
    )
```

```python
import functools
import jax
import jax.numpy as jnp
from jax import lax
from jax.experimental import pallas as pl
from jax.experimental.pallas import tpu as pltpu
from jax.sharding import PartitionSpec as P

SUBSTEPS = 6
ACCEL = 0.3
SPREAD = 0.3
BUOYANCY = 0.5
UNIT = 1.0 / ACCEL
DEEP = 6
GROUP = 2 * DEEP
ZC = 20
SUBL = 8
LANES = 128
F32 = jnp.float32


def lane_ids():
    return lax.broadcasted_iota(jnp.int32, (SUBL, LANES), 1)


def sub_ids():
    return lax.broadcasted_iota(jnp.int32, (SUBL, LANES), 0)


def lroll(x, shift):
    if isinstance(shift, int):
        shift = shift % LANES
        if shift == 0:
            return x
    return pltpu.roll(x, shift, 1)


def sroll(x, shift):
    return pltpu.roll(x, shift % SUBL, 0)


def pack_slabs(we, sn, west, east, south, north):
    band, m = we.shape[3], we.shape[4]
    xs = sn.shape[3]
    west[...] = jnp.zeros_like(west)
    east[...] = jnp.zeros_like(east)
    south[...] = jnp.zeros_like(south)
    north[...] = jnp.zeros_like(north)
    for f in range(3):
        for z in range(ZC):
            g, c = divmod(z, 4)
            west[0, f, g, 0:band, m * c : m * (c + 1)] = we[0, f, z]
            east[0, f, g, 0:band, m * c : m * (c + 1)] = we[1, f, z]
            t, c = divmod(z, 10)
            lo = GROUP * c
            s_val = sn[0, f, z]
            n_val = sn[1, f, z]
            for rep in range(SUBL // xs):
                rows = slice(xs * rep, xs * (rep + 1))
                south[0, f, t, rows, lo : lo + band] = s_val
                for d in range(band):
                    at = lo + band - 1 - d
                    north[0, f, t, rows, at : at + 1] = n_val[:, d : d + 1]


def blend_pack(n_gx, n_gy, m, xs, band, *refs):
    u, v, p, w, r, rate = refs[:6]
    refs = refs[6:]
    we_own = refs[:2]
    sn_own = refs[2:4]
    we_in = refs[4 : 4 + n_gx - 1]
    sn_in = refs[3 + n_gx : 3 + n_gx + n_gy - 1]
    ub, vb, pb, xa, xb, q, c_out = refs[2 + n_gx + n_gy :]
    gx = lax.axis_index("gx")
    gy = lax.axis_index("gy")
    size_x = u.shape[1]
    blocks = size_x // SUBL
    outs = (ub, vb, pb)
    for src, dst in zip((u, v, p), outs):
        dst[...] = src[...]
    lane = lane_ids()
    sub = sub_ids()

    def band_rows(pieces, f, z):
        g, c = z // 4, z % 4
        val = jnp.zeros((SUBL, LANES), F32)
        for s, piece in enumerate(pieces):
            moved = pltpu.roll(piece[0, f, g], jnp.mod(m * s - m * c, LANES), 1)
            val = jnp.where((lane >= m * s) & (lane < m * (s + 1)), moved, val)
        return val

    @pl.when(gx == 0)
    def _():
        pieces = [we_own[0]] + [we_in[s - 1] for s in range(1, n_gx)]
        rt = rate[0:SUBL, :].astype(F32)
        wt = jnp.maximum(rt - sub.astype(F32), 0.0) / rt

        def body(h, carry):
            for z in [h * 4 + i for i in range(4)]:
                for f in range(3):
                    val = band_rows(pieces, f, z)
                    old = outs[f][z, 0:SUBL, :]
                    outs[f][z, 0:SUBL, :] = old + wt * (val - old)
            return carry

        lax.fori_loop(0, ZC // 4, body, 0)

    @pl.when(gx == n_gx - 1)
    def _():
        pieces = [we_in[n_gx - 2 - s] for s in range(n_gx - 1)] + [we_own[1]]
        rt = rate[size_x - SUBL : size_x, :].astype(F32)
        wt = jnp.maximum(rt - (SUBL - 1 - sub).astype(F32), 0.0) / rt

        def body(h, carry):
            for z in [h * 4 + i for i in range(4)]:
                for f in range(3):
                    val = band_rows(pieces, f, z)
                    turned = sroll(val, 1)
                    turned = jnp.where(sub % 4 == 1, sroll(val, 3), turned)
                    turned = jnp.where(sub % 4 == 2, sroll(val, 5), turned)
                    turned = jnp.where(sub % 4 == 3, sroll(val, 7), turned)
                    old = outs[f][z, size_x - SUBL : size_x, :]
                    outs[f][z, size_x - SUBL : size_x, :] = old + wt * (turned - old)
            return carry

        lax.fori_loop(0, ZC // 4, body, 0)

    per = SUBL // xs

    def side_blend(pieces, first, dist):
        wts = []
        for b in range(blocks):
            rt = rate[SUBL * b : SUBL * (b + 1), :].astype(F32)
            wts.append(jnp.maximum(rt - dist, 0.0) / rt)

        def body(h, carry):
            for z in [h * 5 + i for i in range(5)]:
                t, c = z // 10, z % 10
                shift = jnp.mod(first - GROUP * c + LANES, LANES)
                for f in range(3):
                    for b in range(blocks):
                        val = pieces[b * per][0, f, t]
                        for s in range(1, per):
                            val = jnp.where(sub // xs == s, pieces[b * per + s][0, f, t], val)
                        val = pltpu.roll(val, shift, 1)
                        old = outs[f][z, SUBL * b : SUBL * (b + 1), :]
                        outs[f][z, SUBL * b : SUBL * (b + 1), :] = old + wts[b] * (val - old)
            return carry

        lax.fori_loop(0, ZC // 5, body, 0)

    @pl.when(gy == 0)
    def _():
        pieces = [sn_own[0]] + [sn_in[s - 1] for s in range(1, n_gy)]
        side_blend(pieces, 0, lane.astype(F32))

    @pl.when(gy == n_gy - 1)
    def _():
        pieces = [sn_in[n_gy - 2 - s] for s in range(n_gy - 1)] + [sn_own[1]]
        side_blend(pieces, LANES - band, (LANES - 1 - lane).astype(F32))

    even = (gx % 2) == 0
    top = size_x - SUBL

    def strip_of(blocks_of):
        acc = jnp.zeros((SUBL, LANES), F32)
        for b in range(blocks):
            lo = GROUP * (b + 1)
            moved = lroll(blocks_of(b), lo + DEEP)
            acc = jnp.where((lane >= lo) & (lane < lo + GROUP), moved, acc)
        return acc

    def corner_of(strip, spot, acc):
        o = 2 * GROUP * spot
        acc = jnp.where((lane >= o) & (lane < o + GROUP), lroll(strip, o - GROUP * blocks), acc)
        return jnp.where(
            (lane >= o + GROUP) & (lane < o + 2 * GROUP), lroll(strip, o), acc
        )

    def body(h, carry):
        corners = [jnp.zeros((SUBL, LANES), F32)] * 4
        for c5 in range(5):
            z = h * 5 + c5
            for f, src in enumerate((ub, vb, pb, w)):
                strip = strip_of(lambda b: src[z, SUBL * b : SUBL * (b + 1), :])
                q[0, f * ZC + z] = strip
                corners[f] = corner_of(strip, c5, corners[f])
            u7 = ub[z, top:, :]
            u0 = ub[z, 0:SUBL, :]
            v7 = vb[z, top:, :]
            v0 = vb[z, 0:SUBL, :]
            up7 = ub[z, top - 1 : size_x - 1, :]
            up0 = jnp.where(sub == 0, 0.0, sroll(u0, 1))
            e7 = UNIT * ((u7 - up7) + (v7 - jnp.where(lane == 0, 0.0, lroll(v7, 1))))
            e0 = UNIT * ((u0 - up0) + (v0 - jnp.where(lane == 0, 0.0, lroll(v0, 1))))
            ea = jnp.where(sub < 2, sroll(e7, -3), pb[z, top:, :])
            eb = jnp.where(sub < 3, sroll(e7, -5), w[z, top:, :])
            wa = jnp.where(sub < 6, pb[z, 0:SUBL, :], sroll(e0, 6))
            wb = jnp.where(sub < 5, w[z, 0:SUBL, :], sroll(e0, 3))
            at = 2 * SUBL * c5
            xa[h, at : at + SUBL, :] = jnp.where(even, ea, wa)
            xa[h, at + SUBL : at + 2 * SUBL, :] = jnp.where(even, eb, wb)
            xb[h, at : at + SUBL, :] = jnp.where(even, wa, ea)
            xb[h, at + SUBL : at + 2 * SUBL, :] = jnp.where(even, wb, eb)
            last = ub[z, size_x - 1 : size_x, :]
            xa[h, 80 + c5 : 81 + c5, :] = last
            xb[h, 80 + c5 : 81 + c5, :] = last
        for f in range(4):
            c_out[0, f * (ZC // 5) + h] = corners[f]
        return carry

    lax.fori_loop(0, ZC // 5, body, 0)
    strip = strip_of(lambda b: r[SUBL * b : SUBL * (b + 1), :])
    q[0, 4 * ZC] = strip
    c_out[0, 4 * (ZC // 5)] = corner_of(strip, 0, jnp.zeros((SUBL, LANES), F32))
    east_r = r[size_x - 5 : size_x, :]
    west_r = r[0:5, :]
    ra = jnp.where(even, east_r, west_r)
    rb = jnp.where(even, west_r, east_r)
    for ref, val in ((xa, ra), (xb, rb)):
        ref[0, 85:88, :] = val[0:3]
        ref[1, 85:87, :] = val[3:5]
        ref[1, 87:88, :] = val[4:5]
        ref[2, 85:88, :] = val[0:3]
        ref[3, 85:88, :] = val[0:3]


def substeps(n_gx, n_gy, *refs):
    (ub, vb, pb, w, r, xa, xb, qa, qb, ca, cb, caa, cab, cba, cbb) = refs[:15]
    (u_out, v_out, w_out, p_out) = refs[15:19]
    (PM, PS, FM, WM, GM, QM, LM, SM, KM) = refs[19:]
    levels, size_x = ub.shape[0], ub.shape[1]
    blocks = size_x // SUBL
    full = blocks + 2
    every = range(full + 1)
    gx = lax.axis_index("gx")
    gy = lax.axis_index("gy")
    x_even = (gx % 2) == 0
    y_even = (gy % 2) == 0
    is_w, is_e = gx == 0, gx == n_gx - 1
    is_s, is_n = gy == 0, gy == n_gy - 1
    lane = lane_ids()
    sub = sub_ids()
    within = lane % GROUP
    block_of = lane // GROUP
    low_half = within < DEEP
    rim_lo, rim_hi = within == DEEP - 1, within == DEEP
    zero = jnp.zeros((SUBL, LANES), F32)
    rows = [slice(SUBL * b, SUBL * (b + 1)) for b in range(full + 2)]
    COEF, RINV, STEP = 0, 1, 2

    def strip_from(mine, cw, ce, spot):
        o = 2 * GROUP * spot
        got = jnp.where(block_of == 0, lroll(cw, -o), mine)
        return jnp.where(block_of == full - 1, lroll(ce, GROUP * blocks - o), got)

    def four(k, i):
        aa, ab, ba, bb = caa[k, i], cab[k, i], cba[k, i], cbb[k, i]
        a_s, a_n = jnp.where(y_even, ab, aa), jnp.where(y_even, aa, ab)
        b_s, b_n = jnp.where(y_even, bb, ba), jnp.where(y_even, ba, bb)
        a, b = jnp.where(low_half, a_s, a_n), jnp.where(low_half, b_s, b_n)
        return jnp.where(x_even, b, a), jnp.where(x_even, a, b)

    def strip_at(k, iq, corners, spot):
        a, b = qa[k, iq], qb[k, iq]
        mine = jnp.where(low_half == y_even, b, a)
        return strip_from(mine, corners[0], corners[1], spot)

    def strip_rows(s):
        up = sroll(s, 1)
        up = jnp.where(sub == 0, lroll(up, GROUP), up)
        dn = sroll(s, -1)
        dn = jnp.where(sub == SUBL - 1, lroll(dn, -GROUP), dn)
        return up, dn

    row_first = is_w & (block_of == 1) & (sub == 0)
    row_last = is_e & (block_of == full - 2) & (sub == SUBL - 1)
    lane0, lane_end = lane == 0, lane == LANES - 1
    lane0_in, lane0_rim = lane0 & jnp.logical_not(is_s), lane0 & is_s
    strip_zero = is_n & rim_hi
    fix_w, fix_e = is_w & (sub == SUBL - 1), is_e & (sub == 0)

    def put_pressure(z, tiles):
        tiles = list(tiles)
        tiles[0] = jnp.where(fix_w, sroll(tiles[1], -1), tiles[0])
        tiles[full - 1] = jnp.where(fix_e, 0.0, tiles[full - 1])
        ps = jnp.where(strip_zero, 0.0, tiles[full])
        PS[z] = ps
        s_lf, s_rt = lroll(ps, 1), lroll(ps, -1)
        for b in range(full):
            p0 = tiles[b]
            PM[z, rows[b + 1], :] = p0
            lo = GROUP * b + DEEP
            s_lf = jnp.where(lane == lo, lroll(p0, lo + 1), s_lf)
            s_rt = jnp.where(lane == lo - 1, lroll(p0, lo - 1), s_rt)
            lf = jnp.where(lane0_in, lroll(ps, 1 - lo), lroll(p0, 1))
            lf = jnp.where(lane0_rim, p0, lf)
            rt = jnp.where(lane_end, lroll(ps, -1 - lo), lroll(p0, -1))
            LM[z, rows[b], :] = lf + rt
        up, dn = strip_rows(ps)
        up = jnp.where(row_first, ps, up)
        dn = jnp.where(row_last, 0.0, dn)
        LM[z, rows[full], :] = (s_lf + s_rt) + (up + dn)

    west_x = lambda h, lo, hi: jnp.where(x_even, xb[h, lo:hi, :], xa[h, lo:hi, :])
    east_x = lambda h, lo, hi: jnp.where(x_even, xa[h, lo:hi, :], xb[h, lo:hi, :])
    KM[COEF] = jnp.ones((SUBL * (full + 1), LANES), F32)
    KM[COEF, SUBL : SUBL * (blocks + 1), :] = r[...]
    KM[COEF, 3:6, :] = west_x(0, 85, 88)
    KM[COEF, 6:8, :] = west_x(1, 85, 87)
    lo = SUBL * (full - 1)
    KM[COEF, lo : lo + 3, :] = east_x(0, 85, 88)
    KM[COEF, lo + 3 : lo + 5, :] = east_x(1, 85, 87)
    KM[COEF, rows[full], :] = strip_at(0, 4 * ZC, four(0, 4 * (ZC // 5)), 0)
    kappas, rhos = [], []
    for b in every:
        c = KM[COEF, rows[b], :]
        c = jnp.where(c > 0.0, c, 1.0)
        KM[COEF, rows[b], :] = c
        KM[RINV, rows[b], :] = 1.0 / c
        KM[STEP, rows[b], :] = BUOYANCY / c
        k = 2.0 * c / ((1.0 + 2.0 * c) + jnp.sqrt(1.0 + 4.0 * c))
        kappas.append(k)
        rhos.append(k * k)

    def factor_body(z, carry):
        powers, lows = carry
        new_p, new_l = [], []
        for b in every:
            nxt = powers[b] * rhos[b]
            high = 1.0 - nxt
            GM[z + 1, rows[b], :] = kappas[b] * (lows[b] / high)
            new_p.append(nxt)
            new_l.append(high)
        return tuple(new_p), tuple(new_l)

    lax.fori_loop(0, levels, factor_body, (tuple(rhos), tuple(1.0 - x for x in rhos)))
    wide = jnp.zeros((SUBL * (full + 1), LANES), F32)
    GM[0] = wide
    WM[0] = wide
    QM[levels] = wide
    FM[levels] = wide
    LM[levels] = wide
    PM[levels] = jnp.zeros((SUBL * (full + 2), LANES), F32)
    PS[levels] = zero
    SM[levels] = jnp.zeros((SUBL * (blocks + 2), LANES), F32)

    s5 = ZC // 5

    def unpack(h, carry):
        k, hh = h // s5, h % s5
        corners = [four(k, f * s5 + hh) for f in range(4)]
        i_v = s5 + hh
        v_w = jnp.where(x_even, cb[k, i_v], ca[k, i_v])
        v_e = jnp.where(x_even, ca[k, i_v], cb[k, i_v])
        for c5 in range(5):
            z, zz = h * 5 + c5, hh * 5 + c5
            us, vs, ps, ws = [strip_at(k, f * ZC + zz, corners[f], c5) for f in range(4)]
            at = 2 * SUBL * c5
            xa_a, xa_b = xa[h, at : at + SUBL, :], xa[h, at + SUBL : at + 2 * SUBL, :]
            xb_a, xb_b = xb[h, at : at + SUBL, :], xb[h, at + SUBL : at + 2 * SUBL, :]
            wa, wb = jnp.where(x_even, xb_a, xa_a), jnp.where(x_even, xb_b, xa_b)
            ea, eb = jnp.where(x_even, xa_a, xb_a), jnp.where(x_even, xa_b, xb_b)
            f_west = jnp.where(sub < 5, sroll(wa, 3), sroll(wb, 5))
            f_east = jnp.where(sub < 2, sroll(ea, 2), sroll(eb, -3))
            u_row = jnp.where(x_even, xb[h, 80 + c5 : 81 + c5, :], xa[h, 80 + c5 : 81 + c5, :])
            u_row = jnp.where(is_w, 0.0, u_row)
            vm = [vb[z, rows[b], :] for b in range(blocks)]
            v_left = jnp.where(rim_hi, zero, lroll(vs, 1))
            far = strip_from(zero, v_w, v_e, c5)
            v_left = jnp.where(rim_hi, lroll(far, 1), v_left)
            for b in range(blocks):
                lo = GROUP * (b + 1) + DEEP
                v_left = jnp.where(lane == lo, lroll(vm[b], lo + 1), v_left)
            u_up, _ = strip_rows(us)
            FM[z, rows[full], :] = UNIT * ((us - u_up) + (vs - v_left))
            WM[z + 1, rows[full], :] = ws * KM[RINV, rows[full], :]
            tiles = [wa] + [pb[z, rows[b], :] for b in range(blocks)] + [ea, ps]
            put_pressure(z, tiles)
            for b in range(full):
                v_rim = jnp.where(lane0, lroll(vs, 1 - (GROUP * b + DEEP)), 0.0)
                if b == 0:
                    e, ww = f_west - UNIT * v_rim, wb
                elif b == full - 1:
                    u63 = jnp.where(sub == 0, sroll(ub[z, rows[blocks - 1], :], 1), 0.0)
                    e, ww = f_east - UNIT * (v_rim + u63), eb
                else:
                    m = b - 1
                    uu = ub[z, rows[m], :]
                    if m == 0:
                        up = jnp.where(sub == 0, u_row, sroll(uu, 1))
                    else:
                        up = ub[z, SUBL * m - 1 : SUBL * (m + 1) - 1, :]
                    left = jnp.where(lane0, v_rim, lroll(vm[m], 1))
                    e = UNIT * ((uu - up) + (vm[m] - left))
                    ww = w[z, rows[m], :]
                FM[z, rows[b], :] = e
                WM[z + 1, rows[b], :] = ww * KM[RINV, rows[b], :]
            SM[z] = jnp.zeros((SUBL * (blocks + 2), LANES), F32)
            PM[z, rows[0], :] = zero
            PM[z, rows[full + 1], :] = zero
        return carry

    lax.fori_loop(0, levels // 5, unpack, 0)

    coef_step = ACCEL * SPREAD
    inner = range(1, full - 1)

    def section(z, last):
        qs = {}
        for b in every:
            p0 = PM[z, rows[b + 1], :] if b < full else PS[z]
            if b >= 1:
                SM[z, rows[b - 1], :] += p0
            if last and b not in inner:
                continue
            around = LM[z, rows[b], :]
            if b < full:
                up = PM[z, SUBL * (b + 1) - 1 : SUBL * (b + 2) - 1, :]
                dn = PM[z, SUBL * (b + 1) + 1 : SUBL * (b + 2) + 1, :]
                around = around + (up + dn)
            f = FM[z, rows[b], :] + (4.0 * p0 - around)
            if not last:
                FM[z, rows[b], :] = f
            qq = p0 - coef_step * f
            QM[z, rows[b], :] = qq
            qs[b] = qq
        return qs

    def run_step(last):
        active = inner if last else every

        def forward(i, carry):
            q_here = dict(zip(active, carry[0]))
            d_prev = dict(zip(active, carry[1]))
            for z in (2 * i, 2 * i + 1):
                q_next = section(z + 1, last)
                for b in active:
                    rhs = WM[z + 1, rows[b], :] + KM[STEP, rows[b], :] * (q_here[b] - q_next[b])
                    d = GM[z + 1, rows[b], :] * (rhs + d_prev[b])
                    WM[z + 1, rows[b], :] = d
                    d_prev[b] = d
                q_here = q_next
            return tuple(q_here[b] for b in active), tuple(d_prev[b] for b in active)

        q0 = section(0, last)
        start = (tuple(q0[b] for b in active), tuple(zero for _ in active))
        _, tops = lax.fori_loop(0, levels // 2, forward, start)
        if not last:
            for b, top in zip(active, tops):
                WM[levels, rows[b], :] = top * KM[RINV, rows[b], :]

        def backward(i, above):
            above = dict(zip(active, above))
            for c in range(4):
                z = levels - 1 - (4 * i + c)
                tiles = {}
                below = {}
                for b in active:
                    ww = WM[z, rows[b], :] + GM[z, rows[b], :] * above[b]
                    tiles[b] = QM[z, rows[b], :] - BUOYANCY * (above[b] - ww)
                    if not last:
                        WM[z, rows[b], :] = ww * KM[RINV, rows[b], :]
                    below[b] = ww
                if last:
                    ss = SM[z, rows[blocks + 1], :]
                    for b in active:
                        m = rows[b - 1]
                        w_out[z, m, :] = above[b]
                        p_out[z, m, :] = tiles[b]
                        s0 = SM[z, m, :]
                        dn = SM[z, SUBL * (b - 1) + 1 : SUBL * b + 1, :]
                        rt = jnp.where(
                            lane_end, lroll(ss, -1 - (GROUP * b + DEEP)), lroll(s0, -1)
                        )
                        u_out[z, m, :] = ub[z, m, :] - ACCEL * (dn - s0)
                        v_out[z, m, :] = vb[z, m, :] - ACCEL * (rt - s0)
                else:
                    put_pressure(z, [tiles[b] for b in every])
                above = below
            return tuple(above[b] for b in active)

        lax.fori_loop(0, levels // 4, backward, tops)

    def step(_, carry):
        run_step(False)
        return carry

    lax.fori_loop(0, SUBSTEPS - 1, step, 0)
    run_step(True)


def swap(block, axis, second):
    n = lax.axis_size(axis)
    return lax.ppermute(block, axis, pairing(n, second))


def pairing(n, second):
    lo = 1 if second else 0
    pairs = []
    for i in range(lo, n - 1, 2):
        pairs += [(i, i + 1), (i + 1, i)]
    return pairs


def swap2(block, second_x, second_y):
    nx, ny = lax.axis_size("gx"), lax.axis_size("gy")
    pairs = []
    for a, b in pairing(nx, second_x):
        for c, d in pairing(ny, second_y):
            pairs.append((a * ny + c, b * ny + d))
    return lax.ppermute(block, ("gx", "gy"), pairs)


def to_ends(low, high, axis):
    n = lax.axis_size(axis)
    me = lax.axis_index(axis)
    got = []
    for k in range(1, n):
        block = jnp.where(me == k, low, high)
        got.append(lax.ppermute(block, axis, [(k, 0), (n - 1 - k, n - 1)]))
    return got


def per_device(u_wind, v_wind, w_wind, pressure, vert_coef, we_slab, sn_slab, relax_width):
    n_gx, n_gy = lax.axis_size("gx"), lax.axis_size("gy")
    levels, size_x, size_y = pressure.shape
    blocks = size_x // SUBL
    full = blocks + 2
    band, m = we_slab.shape[3], we_slab.shape[4]
    xs = sn_slab.shape[4]
    steps = levels // ZC
    sds = jax.ShapeDtypeStruct
    big = pltpu.CompilerParams(vmem_limit_bytes=60 * 1024 * 1024)

    sn_t = jnp.transpose(sn_slab, (0, 1, 2, 4, 3))
    we_shape = (steps, 3, ZC // 4, SUBL, LANES)
    sn_shape = (steps, 3, ZC // 10, SUBL, LANES)
    lead = lambda shape: pl.BlockSpec((1,) + shape[1:], lambda i: (i,) + (0,) * (len(shape) - 1))
    west, east, south, north = pl.pallas_call(
        pack_slabs,
        grid=(steps,),
        in_specs=[
            pl.BlockSpec((2, 3, ZC, band, m), lambda i: (0, 0, i, 0, 0)),
            pl.BlockSpec((2, 3, ZC, xs, band), lambda i: (0, 0, i, 0, 0)),
        ],
        out_specs=[lead(we_shape)] * 2 + [lead(sn_shape)] * 2,
        out_shape=[sds(we_shape, F32)] * 2 + [sds(sn_shape, F32)] * 2,
        name="pack_slabs",
    )(we_slab, sn_t)
    we_in = to_ends(west, east, "gx")
    sn_in = to_ends(south, north, "gy")

    field = pl.BlockSpec((ZC, size_x, size_y), lambda i: (i, 0, 0))
    plane = pl.BlockSpec((size_x, size_y), lambda i: (0, 0))
    x_shape = (levels // 5, 88, LANES)
    q_shape = (steps, 4 * ZC + 1, SUBL, LANES)
    c_shape = (steps, 4 * (ZC // 5) + 1, SUBL, LANES)
    ub, vb, pb, xa, xb, q, c = pl.pallas_call(
        functools.partial(blend_pack, n_gx, n_gy, m, xs, band),
        grid=(steps,),
        in_specs=[field] * 4
        + [plane] * 2
        + [lead(we_shape)] * 2
        + [lead(sn_shape)] * 2
        + [lead(we_shape)] * (n_gx - 1)
        + [lead(sn_shape)] * (n_gy - 1),
        out_specs=[field] * 3
        + [pl.BlockSpec((ZC // 5, 88, LANES), lambda i: (i, 0, 0))] * 2
        + [lead(q_shape), lead(c_shape)],
        out_shape=[sds(pressure.shape, F32)] * 3
        + [sds(x_shape, F32)] * 2
        + [sds(q_shape, F32), sds(c_shape, F32)],
        compiler_params=big,
        name="blend_pack",
    )(
        u_wind, v_wind, pressure, w_wind, vert_coef, relax_width,
        west, east, south, north, *we_in, *sn_in,
    )
    xa = swap(xa, "gx", False)
    xb = swap(xb, "gx", True)
    qa = swap(q, "gy", False)
    qb = swap(q, "gy", True)
    ca = swap(c, "gx", False)
    cb = swap(c, "gx", True)
    caa = swap2(c, False, False)
    cab = swap2(c, False, True)
    cba = swap2(c, True, False)
    cbb = swap2(c, True, True)

    whole = pl.BlockSpec(memory_space=pltpu.VMEM)
    tall = pltpu.VMEM((levels + 1, SUBL * (full + 1), LANES), F32)
    return pl.pallas_call(
        functools.partial(substeps, n_gx, n_gy),
        in_specs=[whole] * 15,
        out_specs=[whole] * 4,
        out_shape=[sds(pressure.shape, F32)] * 4,
        scratch_shapes=[
            pltpu.VMEM((levels + 1, SUBL * (full + 2), LANES), F32),
            pltpu.VMEM((levels + 1, SUBL, LANES), F32),
            tall, tall, tall, tall, tall,
            pltpu.VMEM((levels + 1, SUBL * (blocks + 2), LANES), F32),
            pltpu.VMEM((3, SUBL * (full + 1), LANES), F32),
        ],
        compiler_params=big,
        name="substeps",
    )(ub, vb, pb, w_wind, vert_coef, xa, xb, qa, qb, ca, cb, caa, cab, cba, cbb)


def solution(mesh):
    cell = P(None, "gx", "gy")
    placed = (
        cell, cell, cell, cell,
        P("gx", "gy"),
        P(None, None, None, None, ("gy", "gx")),
        P(None, None, None, None, ("gx", "gy")),
        P("gx", "gy"),
    )
    return jax.shard_map(
        per_device,
        mesh=mesh,
        in_specs=placed,
        out_specs=(cell, cell, cell, cell),
        check_vma=False,
    )
```

```python
import functools
import jax
import jax.numpy as jnp
from jax import lax
from jax.experimental import pallas as pl
from jax.experimental.pallas import tpu as pltpu
from jax.sharding import PartitionSpec as P

SUBSTEPS = 6
ACCEL = 0.3
SPREAD = 0.3
BUOYANCY = 0.5
UNIT = 1.0 / ACCEL
DEEP = 6
GROUP = 2 * DEEP
ZC = 20
SUBL = 8
LANES = 128
F32 = jnp.float32


def lane_ids():
    return lax.broadcasted_iota(jnp.int32, (SUBL, LANES), 1)


def sub_ids():
    return lax.broadcasted_iota(jnp.int32, (SUBL, LANES), 0)


def lroll(x, shift):
    if isinstance(shift, int):
        shift = shift % LANES
        if shift == 0:
            return x
    return pltpu.roll(x, shift, 1)


def sroll(x, shift):
    return pltpu.roll(x, shift % SUBL, 0)


SLOT = 25


def pack_slabs(n_gx, n_gy, we, sn, *refs):
    we_own, sn_own = refs[0], refs[n_gx]
    we_out, sn_out = refs[1:n_gx], refs[n_gx + 1 : n_gx + n_gy]
    tile, flat = refs[n_gx + n_gy :]
    gx = lax.axis_index("gx")
    gy = lax.axis_index("gy")
    band, m, levels = we.shape[2:]
    xs = sn.shape[3]
    groups = we_own.shape[0]
    slots = sn_own.shape[1]
    tile[...] = jnp.zeros_like(tile)
    flat[...] = jnp.zeros_like(flat)
    for g in range(groups):
        for side in range(2):
            for c in range(4):
                fd = 4 * g + c
                if fd < 3 * band:
                    tile[side, m * c : m * (c + 1), 0:levels] = we[side, fd // band, fd % band]
        west = tile[0].T[0 : we_own.shape[1]]
        east = tile[1].T[0 : we_own.shape[1]]
        we_own[g] = jnp.where(gx == 0, west, east)
        for k, ref in enumerate(we_out):
            ref[g] = jnp.where(gx == k + 1, west, east)
    level = lax.broadcasted_iota(jnp.int32, (LANES, LANES), 0)
    lane = lax.broadcasted_iota(jnp.int32, (LANES, LANES), 1)
    for f in range(3):
        for side in range(2):
            for d in range(band):
                for rep in range(SUBL // xs):
                    lo = SUBL * f + xs * rep
                    flat[side, d, lo : lo + xs, 0:levels] = sn[side, f, d]
    for t in range(slots):
        vals = []
        for side in range(2):
            acc = jnp.zeros((3 * SUBL, LANES), F32)
            for d in range(band):
                at = d if side == 0 else band - 1 - d
                put = (lane == band * (level - SLOT * t) + at) & (level >= SLOT * t)
                put = put & (level < SLOT * (t + 1))
                acc = acc + jnp.dot(
                    flat[side, d],
                    put.astype(F32),
                    precision=lax.Precision.HIGHEST,
                    preferred_element_type=F32,
                )
            vals.append(acc)
        for f in range(3):
            south = vals[0][SUBL * f : SUBL * (f + 1)]
            north = vals[1][SUBL * f : SUBL * (f + 1)]
            sn_own[f, t] = jnp.where(gy == 0, south, north)
            for k, ref in enumerate(sn_out):
                ref[f, t] = jnp.where(gy == k + 1, south, north)


def pack_rows(size_x, u0, u7, v0, v7, p0, p7, w0, w7, r, xa, xb):
    even = (lax.axis_index("gx") % 2) == 0
    lane = lane_ids()
    sub = sub_ids()

    def body(h, carry):
        for c5 in range(5):
            z = h * 5 + c5
            ut, ub, vt, vb = u7[z], u0[z], v7[z], v0[z]
            e7 = UNIT * ((ut - sroll(ut, 1)) + (vt - jnp.where(lane == 0, 0.0, lroll(vt, 1))))
            up0 = jnp.where(sub == 0, 0.0, sroll(ub, 1))
            e0 = UNIT * ((ub - up0) + (vb - jnp.where(lane == 0, 0.0, lroll(vb, 1))))
            ea = jnp.where(sub < 2, sroll(e7, -3), p7[z])
            eb = jnp.where(sub < 3, sroll(e7, -5), w7[z])
            wa = jnp.where(sub < 6, p0[z], sroll(e0, 6))
            wb = jnp.where(sub < 5, w0[z], sroll(e0, 3))
            at = 2 * SUBL * c5
            xa[h, at : at + SUBL, :] = jnp.where(even, ea, wa)
            xa[h, at + SUBL : at + 2 * SUBL, :] = jnp.where(even, eb, wb)
            xb[h, at : at + SUBL, :] = jnp.where(even, wa, ea)
            xb[h, at + SUBL : at + 2 * SUBL, :] = jnp.where(even, wb, eb)
            last = ut[SUBL - 1 : SUBL, :]
            xa[h, 80 + c5 : 81 + c5, :] = last
            xb[h, 80 + c5 : 81 + c5, :] = last
        return carry

    lax.fori_loop(0, xa.shape[0], body, 0)
    east_r = r[size_x - 5 : size_x, :]
    west_r = r[0:5, :]
    ra = jnp.where(even, east_r, west_r)
    rb = jnp.where(even, west_r, east_r)
    for ref, val in ((xa, ra), (xb, rb)):
        ref[0, 85:88, :] = val[0:3]
        ref[1, 85:87, :] = val[3:5]
        ref[1, 87:88, :] = val[4:5]
        ref[2, 85:88, :] = val[0:3]
        ref[3, 85:88, :] = val[0:3]


def blend_pack(n_gx, n_gy, m, xs, band, *refs):
    u, v, p, w, r, rate = refs[:6]
    refs = refs[6:]
    we_own, sn_own = refs[0], refs[n_gx]
    we_in = refs[1:n_gx]
    sn_in = refs[n_gx + 1 : n_gx + n_gy]
    ub, vb, pb, q, ca, cb, daa, dab, dba, dbb, rows_we, corners = refs[n_gx + n_gy :]
    gx = lax.axis_index("gx")
    gy = lax.axis_index("gy")
    chunk = pl.program_id(0)
    size_x = u.shape[1]
    blocks = size_x // SUBL
    outs = (ub, vb, pb)
    for src, dst in zip((u, v, p), outs):
        dst[...] = src[...]
    lane = lane_ids()
    sub = sub_ids()

    def band_blend(pieces, row_of):
        tall_lane = lax.broadcasted_iota(jnp.int32, rows_we.shape[1:], 1)

        @pl.when(chunk == 0)
        def _():
            for fd in range(3 * band):
                g, c = divmod(fd, 4)
                val = None
                for s, piece in enumerate(pieces):
                    moved = lroll(piece[g], m * (s - c))
                    if val is None:
                        val = moved
                    else:
                        val = jnp.where(tall_lane >= m * s, moved, val)
                rows_we[fd] = val

        wts = []
        for d in range(band):
            rt = rate[row_of(d) : row_of(d) + 1, :].astype(F32)
            wts.append(jnp.maximum(rt - float(d), 0.0) / rt)

        def body(h, carry):
            for i in range(5):
                z = h * 5 + i
                for f in range(3):
                    for d in range(band):
                        at = slice(row_of(d), row_of(d) + 1)
                        val = rows_we[f * band + d, pl.ds(chunk * ZC + z, 1), :]
                        old = outs[f][z, at, :]
                        outs[f][z, at, :] = old + wts[d] * (val - old)
            return carry

        lax.fori_loop(0, ZC // 5, body, 0)

    @pl.when(gx == 0)
    def _():
        band_blend([we_own] + [we_in[s - 1] for s in range(1, n_gx)], lambda d: d)

    @pl.when(gx == n_gx - 1)
    def _():
        band_blend(
            [we_in[n_gx - 2 - s] for s in range(n_gx - 1)] + [we_own],
            lambda d: size_x - 1 - d,
        )

    per = SUBL // xs

    def side_blend(pieces, first, dist):
        wts = []
        for b in range(blocks):
            rt = rate[SUBL * b : SUBL * (b + 1), :].astype(F32)
            wts.append(jnp.maximum(rt - dist, 0.0) / rt)

        def body(h, carry):
            for z in [h * 5 + i for i in range(5)]:
                t, c = (chunk * ZC + z) // SLOT, (chunk * ZC + z) % SLOT
                shift = jnp.mod(first - band * c + LANES, LANES)
                for f in range(3):
                    for b in range(blocks):
                        val = pieces[b * per][f, t]
                        for s in range(1, per):
                            val = jnp.where(sub // xs == s, pieces[b * per + s][f, t], val)
                        val = pltpu.roll(val, shift, 1)
                        old = outs[f][z, SUBL * b : SUBL * (b + 1), :]
                        outs[f][z, SUBL * b : SUBL * (b + 1), :] = old + wts[b] * (val - old)
            return carry

        lax.fori_loop(0, ZC // 5, body, 0)

    @pl.when(gy == 0)
    def _():
        side_blend([sn_own] + [sn_in[s - 1] for s in range(1, n_gy)], 0, lane.astype(F32))

    @pl.when(gy == n_gy - 1)
    def _():
        side_blend(
            [sn_in[n_gy - 2 - s] for s in range(n_gy - 1)] + [sn_own],
            LANES - band,
            (LANES - 1 - lane).astype(F32),
        )

    def strip_of(blocks_of):
        acc = jnp.zeros((SUBL, LANES), F32)
        for b in range(blocks):
            lo = GROUP * (b + 1)
            moved = lroll(blocks_of(b), lo + DEEP)
            acc = jnp.where((lane >= lo) & (lane < lo + GROUP), moved, acc)
        return acc

    x_even = (gx % 2) == 0
    y_even = (gy % 2) == 0
    bases = [
        jnp.where(x_even, LANES - GROUP * blocks, LANES - GROUP),
        jnp.where(x_even, LANES - GROUP, LANES - GROUP * blocks),
    ]

    def body(t, carry):
        for f, src in enumerate((ub, vb, pb, w)):
            strips = []
            for c in range(10):
                z = t * 10 + c
                strip = strip_of(lambda b: src[z, SUBL * b : SUBL * (b + 1), :])
                q[0, f * ZC + z] = strip
                strips.append(strip)
            for side in range(2):
                acc = jnp.zeros((SUBL, LANES), F32)
                for c in range(10):
                    moved = pltpu.roll(strips[c], jnp.mod(bases[side] + GROUP * c, LANES), 1)
                    here = (lane >= GROUP * c) & (lane < GROUP * (c + 1))
                    acc = jnp.where(here, moved, acc)
                corners[side, f, t] = acc
        return carry

    lax.fori_loop(0, ZC // 10, body, 0)
    strip = strip_of(lambda b: r[SUBL * b : SUBL * (b + 1), :])
    q[0, 4 * ZC] = strip
    low_half = lane % GROUP < DEEP
    for side, near, diag in ((0, ca, (daa, dab)), (1, cb, (dba, dbb))):
        corners[side, 4, 0] = pltpu.roll(strip, bases[side], 1)
        corners[side, 4, 1] = corners[side, 4, 0]
        for f in range(3):
            for t in range(2):
                near[0, 2 * f + t] = corners[side, f, t]
        for way, out in enumerate(diag):
            high = y_even if way == 0 else jnp.logical_not(y_even)
            first = jnp.where(high, 0, LANES - DEEP)
            second = jnp.where(high, DEEP, 0)
            for f in range(5):
                a = pltpu.roll(corners[side, f, 0], first, 1)
                b = pltpu.roll(corners[side, f, 1], second, 1)
                out[0, f] = jnp.where(low_half, a, b)


def substeps(n_gx, n_gy, *refs):
    (ub, vb, pb, w, r, xa, xb, qa, qb, ca, cb, caa, cab, cba, cbb) = refs[:15]
    (u_out, v_out, w_out, p_out) = refs[15:19]
    (PM, PS, FM, WM, GM, QM, LM, SM, KM) = refs[19:]
    levels, size_x = ub.shape[0], ub.shape[1]
    blocks = size_x // SUBL
    full = blocks + 2
    every = range(full + 1)
    gx = lax.axis_index("gx")
    gy = lax.axis_index("gy")
    x_even = (gx % 2) == 0
    y_even = (gy % 2) == 0
    is_w, is_e = gx == 0, gx == n_gx - 1
    is_s, is_n = gy == 0, gy == n_gy - 1
    lane = lane_ids()
    sub = sub_ids()
    within = lane % GROUP
    block_of = lane // GROUP
    low_half = within < DEEP
    rim_lo, rim_hi = within == DEEP - 1, within == DEEP
    zero = jnp.zeros((SUBL, LANES), F32)
    rows = [slice(SUBL * b, SUBL * (b + 1)) for b in range(full + 2)]
    COEF, RINV, STEP = 0, 1, 2

    def strip_from(mine, cw, ce, spot):
        west = pltpu.roll(cw, jnp.mod(LANES - GROUP * spot, LANES), 1)
        east = pltpu.roll(ce, jnp.mod(LANES + GROUP * (full - 1) - GROUP * spot, LANES), 1)
        got = jnp.where(block_of == 0, west, mine)
        return jnp.where(block_of == full - 1, east, got)

    def four(k, i, late):
        aa, ab, ba, bb = caa[k, i], cab[k, i], cba[k, i], cbb[k, i]
        back = jnp.where(late, LANES - DEEP, 0)
        ahead = jnp.where(late, 0, DEEP)
        pairs = []
        for sa, sb in ((aa, ab), (ba, bb)):
            south, north = jnp.where(y_even, sb, sa), jnp.where(y_even, sa, sb)
            south, north = pltpu.roll(south, back, 1), pltpu.roll(north, ahead, 1)
            pairs.append(jnp.where(low_half, south, north))
        a, b = pairs
        return jnp.where(x_even, b, a), jnp.where(x_even, a, b)

    def strip_at(k, iq, corners, spot):
        a, b = qa[k, iq], qb[k, iq]
        mine = jnp.where(low_half == y_even, b, a)
        return strip_from(mine, corners[0], corners[1], spot)

    def strip_rows(s):
        up = sroll(s, 1)
        up = jnp.where(sub == 0, lroll(up, GROUP), up)
        dn = sroll(s, -1)
        dn = jnp.where(sub == SUBL - 1, lroll(dn, -GROUP), dn)
        return up, dn

    row_first = is_w & (block_of == 1) & (sub == 0)
    row_last = is_e & (block_of == full - 2) & (sub == SUBL - 1)
    lane0, lane_end = lane == 0, lane == LANES - 1
    lane0_in, lane0_rim = lane0 & jnp.logical_not(is_s), lane0 & is_s
    strip_zero = is_n & rim_hi
    fix_w, fix_e = is_w & (sub == SUBL - 1), is_e & (sub == 0)

    def put_pressure(z, tiles):
        tiles = list(tiles)
        tiles[0] = jnp.where(fix_w, sroll(tiles[1], -1), tiles[0])
        tiles[full - 1] = jnp.where(fix_e, 0.0, tiles[full - 1])
        ps = jnp.where(strip_zero, 0.0, tiles[full])
        PS[z] = ps
        rims = zero
        for b in range(full):
            p0 = tiles[b]
            PM[z, rows[b + 1], :] = p0
            lo = GROUP * b + DEEP
            rims = jnp.where((lane == lo) | (lane == lo - 1), lroll(p0, lo), rims)
            LM[z, rows[b], :] = lroll(ps, -lo)
        s_lf = lroll(jnp.where(rim_lo, rims, ps), 1)
        s_rt = lroll(jnp.where(rim_hi, rims, ps), -1)
        up, dn = strip_rows(ps)
        up = jnp.where(row_first, ps, up)
        dn = jnp.where(row_last, 0.0, dn)
        LM[z, rows[full], :] = (s_lf + s_rt) + (up + dn)

    west_x = lambda h, lo, hi: jnp.where(x_even, xb[h, lo:hi, :], xa[h, lo:hi, :])
    east_x = lambda h, lo, hi: jnp.where(x_even, xa[h, lo:hi, :], xb[h, lo:hi, :])
    KM[COEF] = jnp.ones((SUBL * (full + 1), LANES), F32)
    KM[COEF, SUBL : SUBL * (blocks + 1), :] = r[...]
    KM[COEF, 3:6, :] = west_x(0, 85, 88)
    KM[COEF, 6:8, :] = west_x(1, 85, 87)
    lo = SUBL * (full - 1)
    KM[COEF, lo : lo + 3, :] = east_x(0, 85, 88)
    KM[COEF, lo + 3 : lo + 5, :] = east_x(1, 85, 87)
    KM[COEF, rows[full], :] = strip_at(0, 4 * ZC, four(0, 4, False), 0)
    kappas, rhos = [], []
    for b in every:
        c = KM[COEF, rows[b], :]
        c = jnp.where(c > 0.0, c, 1.0)
        KM[COEF, rows[b], :] = c
        KM[RINV, rows[b], :] = 1.0 / c
        KM[STEP, rows[b], :] = BUOYANCY / c
        k = 2.0 * c / ((1.0 + 2.0 * c) + jnp.sqrt(1.0 + 4.0 * c))
        kappas.append(k)
        rhos.append(k * k)

    def factor_body(z, carry):
        powers, lows = carry
        new_p, new_l = [], []
        for b in every:
            nxt = powers[b] * rhos[b]
            high = 1.0 - nxt
            GM[z + 1, rows[b], :] = kappas[b] * (lows[b] / high)
            new_p.append(nxt)
            new_l.append(high)
        return tuple(new_p), tuple(new_l)

    lax.fori_loop(0, levels, factor_body, (tuple(rhos), tuple(1.0 - x for x in rhos)))
    wide = jnp.zeros((SUBL * (full + 1), LANES), F32)
    GM[0] = wide
    WM[0] = wide
    for z in range(levels, FM.shape[0]):
        FM[z] = wide
        LM[z] = wide
        PM[z] = jnp.zeros((SUBL * (full + 2), LANES), F32)
        PS[z] = zero
        SM[z] = jnp.zeros((SUBL * (blocks + 2), LANES), F32)

    s5 = ZC // 5

    def patch(near, side, spot, p_old, f_old):
        shift = jnp.mod(LANES - GROUP * spot - DEEP, LANES)
        uu, vv, pp = [pltpu.roll(near[f][side], shift, 1) for f in range(3)]
        up = sroll(uu, 1)
        if side == 1:
            up = jnp.where(sub == 0, 0.0, up)
        f_new = UNIT * ((uu - up) + (vv - jnp.where(lane0, 0.0, lroll(vv, 1))))
        mine_s, mine_n = is_s & (lane < DEEP), is_n & (lane > LANES - DEEP)
        here = mine_s | mine_n
        return jnp.where(here, pp, p_old), jnp.where(here, f_new, f_old), (here, uu)

    def unpack(patched, h, carry):
        k, hh = h // s5, h % s5
        late = hh // 2
        corners = [four(k, f, late == 1) for f in range(4)]
        near = []
        for f in range(3):
            a, b = ca[k, 2 * f + late], cb[k, 2 * f + late]
            near.append((jnp.where(x_even, b, a), jnp.where(x_even, a, b)))
        v_w, v_e = near[1]
        for c5 in range(5):
            z, zz = h * 5 + c5, hh * 5 + c5
            spot = (hh % 2) * 5 + c5
            us, vs, ps, ws = [strip_at(k, f * ZC + zz, corners[f], spot) for f in range(4)]
            at = 2 * SUBL * c5
            xa_a, xa_b = xa[h, at : at + SUBL, :], xa[h, at + SUBL : at + 2 * SUBL, :]
            xb_a, xb_b = xb[h, at : at + SUBL, :], xb[h, at + SUBL : at + 2 * SUBL, :]
            wa, wb = jnp.where(x_even, xb_a, xa_a), jnp.where(x_even, xb_b, xa_b)
            ea, eb = jnp.where(x_even, xa_a, xb_a), jnp.where(x_even, xa_b, xb_b)
            f_west = jnp.where(sub < 5, sroll(wa, 3), sroll(wb, 5))
            f_east = jnp.where(sub < 2, sroll(ea, 2), sroll(eb, -3))
            u_side = None
            if patched:
                wa, f_west, u_side = patch(near, 0, spot, wa, f_west)
                ea, f_east, _ = patch(near, 1, spot, ea, f_east)
            u_row = jnp.where(x_even, xb[h, 80 + c5 : 81 + c5, :], xa[h, 80 + c5 : 81 + c5, :])
            if u_side is not None:
                here, uu = u_side
                u_row = jnp.where(here, sroll(uu, 1), u_row)
            u_row = jnp.where(is_w, 0.0, u_row)
            vm = [vb[z, rows[b], :] for b in range(blocks)]
            v_left = jnp.where(rim_hi, zero, lroll(vs, 1))
            far = strip_from(zero, v_w, v_e, spot)
            v_left = jnp.where(rim_hi, lroll(far, 1), v_left)
            for b in range(blocks):
                lo = GROUP * (b + 1) + DEEP
                v_left = jnp.where(lane == lo, lroll(vm[b], lo + 1), v_left)
            u_up, _ = strip_rows(us)
            FM[z, rows[full], :] = UNIT * ((us - u_up) + (vs - v_left))
            WM[z + 1, rows[full], :] = ws * KM[RINV, rows[full], :]
            tiles = [wa] + [pb[z, rows[b], :] for b in range(blocks)] + [ea, ps]
            put_pressure(z, tiles)
            for b in range(full):
                v_rim = jnp.where(lane0, lroll(vs, 1 - (GROUP * b + DEEP)), 0.0)
                if b == 0:
                    e, ww = f_west - UNIT * v_rim, wb
                elif b == full - 1:
                    u63 = jnp.where(sub == 0, sroll(ub[z, rows[blocks - 1], :], 1), 0.0)
                    e, ww = f_east - UNIT * (v_rim + u63), eb
                else:
                    m = b - 1
                    uu = ub[z, rows[m], :]
                    if m == 0:
                        up = jnp.where(sub == 0, u_row, sroll(uu, 1))
                    else:
                        up = ub[z, SUBL * m - 1 : SUBL * (m + 1) - 1, :]
                    left = jnp.where(lane0, v_rim, lroll(vm[m], 1))
                    e = UNIT * ((uu - up) + (vm[m] - left))
                    ww = w[z, rows[m], :]
                FM[z, rows[b], :] = e
                WM[z + 1, rows[b], :] = ww * KM[RINV, rows[b], :]
            SM[z] = jnp.zeros((SUBL * (blocks + 2), LANES), F32)
            PM[z, rows[0], :] = zero
            PM[z, rows[full + 1], :] = zero
        return carry

    rim = is_s | is_n

    @pl.when(rim)
    def _():
        lax.fori_loop(0, levels // 5, functools.partial(unpack, True), 0)

    @pl.when(jnp.logical_not(rim))
    def _():
        lax.fori_loop(0, levels // 5, functools.partial(unpack, False), 0)

    coef_step = ACCEL * SPREAD
    inner = range(1, full - 1)

    def section(z, last):
        for b in every:
            p0 = PM[z, rows[b + 1], :] if b < full else PS[z]
            if b >= 1:
                SM[z, rows[b - 1], :] += p0
            if last and b not in inner:
                continue
            around = LM[z, rows[b], :]
            if b < full:
                lf = lroll(jnp.where(lane_end, around, p0), 1)
                lf = jnp.where(lane0_rim, p0, lf)
                rt = lroll(jnp.where(lane0, around, p0), -1)
                up = PM[z, SUBL * (b + 1) - 1 : SUBL * (b + 2) - 1, :]
                dn = PM[z, SUBL * (b + 1) + 1 : SUBL * (b + 2) + 1, :]
                around = (lf + rt) + (up + dn)
            f = FM[z, rows[b], :] + (4.0 * p0 - around)
            if not last:
                FM[z, rows[b], :] = f
            QM[z, rows[b], :] = p0 - coef_step * f

    def run_step(last):
        active = inner if last else every
        for z in range(5):
            section(z, last)

        def forward(i, carry):
            d_prev = dict(zip(active, carry))
            for c in range(4):
                section(4 * i + 5 + c, last)
            for c in range(4):
                z = 4 * i + c
                for b in active:
                    change = QM[z, rows[b], :] - QM[z + 1, rows[b], :]
                    rhs = WM[z + 1, rows[b], :] + KM[STEP, rows[b], :] * change
                    d = GM[z + 1, rows[b], :] * (rhs + d_prev[b])
                    WM[z + 1, rows[b], :] = d
                    d_prev[b] = d
            return tuple(d_prev[b] for b in active)

        tops = lax.fori_loop(0, levels // 4, forward, tuple(zero for _ in active))
        if not last:
            for b, top in zip(active, tops):
                WM[levels, rows[b], :] = top * KM[RINV, rows[b], :]

        def backward(i, above):
            above = dict(zip(active, above))
            for c in range(4):
                z = levels - 1 - (4 * i + c)
                tiles = {}
                below = {}
                for b in active:
                    ww = WM[z, rows[b], :] + GM[z, rows[b], :] * above[b]
                    tiles[b] = QM[z, rows[b], :] - BUOYANCY * (above[b] - ww)
                    if not last:
                        WM[z, rows[b], :] = ww * KM[RINV, rows[b], :]
                    below[b] = ww
                if last:
                    ss = SM[z, rows[blocks + 1], :]
                    for b in active:
                        m = rows[b - 1]
                        w_out[z, m, :] = above[b]
                        p_out[z, m, :] = tiles[b]
                        s0 = SM[z, m, :]
                        dn = SM[z, SUBL * (b - 1) + 1 : SUBL * b + 1, :]
                        rt = jnp.where(
                            lane_end, lroll(ss, -1 - (GROUP * b + DEEP)), lroll(s0, -1)
                        )
                        u_out[z, m, :] = ub[z, m, :] - ACCEL * (dn - s0)
                        v_out[z, m, :] = vb[z, m, :] - ACCEL * (rt - s0)
                else:
                    put_pressure(z, [tiles[b] for b in every])
                above = below
            return tuple(above[b] for b in active)

        lax.fori_loop(0, levels // 4, backward, tops)

    def step(_, carry):
        run_step(False)
        return carry

    lax.fori_loop(0, SUBSTEPS - 1, step, 0)
    run_step(True)


def swap(block, axis, second):
    n = lax.axis_size(axis)
    return lax.ppermute(block, axis, pairing(n, second))


def pairing(n, second):
    lo = 1 if second else 0
    pairs = []
    for i in range(lo, n - 1, 2):
        pairs += [(i, i + 1), (i + 1, i)]
    return pairs


def swap2(block, second_x, second_y):
    nx, ny = lax.axis_size("gx"), lax.axis_size("gy")
    pairs = []
    for a, b in pairing(nx, second_x):
        for c, d in pairing(ny, second_y):
            pairs.append((a * ny + c, b * ny + d))
    return lax.ppermute(block, ("gx", "gy"), pairs)


def to_ends(own, blocks, axis):
    n = lax.axis_size(axis)
    got = [own]
    for k, block in enumerate(blocks, 1):
        got.append(lax.ppermute(block, axis, [(k, 0), (n - 1 - k, n - 1)]))
    return got


def per_device(u_wind, v_wind, w_wind, pressure, vert_coef, we_slab, sn_slab, relax_width):
    n_gx, n_gy = lax.axis_size("gx"), lax.axis_size("gy")
    levels, size_x, size_y = pressure.shape
    blocks = size_x // SUBL
    full = blocks + 2
    band, m = we_slab.shape[3], we_slab.shape[4]
    xs = sn_slab.shape[4]
    steps = levels // ZC
    sds = jax.ShapeDtypeStruct
    big = pltpu.CompilerParams(vmem_limit_bytes=60 * 1024 * 1024)
    vmem = pl.BlockSpec(memory_space=pltpu.VMEM)

    lead = lambda shape: pl.BlockSpec((1,) + shape[1:], lambda i: (i,) + (0,) * (len(shape) - 1))
    fixed = lambda shape: pl.BlockSpec(shape, lambda i: (0,) * len(shape))
    field = pl.BlockSpec((ZC, size_x, size_y), lambda i: (i, 0, 0))
    low = pl.BlockSpec((ZC, SUBL, size_y), lambda i: (i, 0, 0))
    high = pl.BlockSpec((ZC, SUBL, size_y), lambda i: (i, blocks - 1, 0))
    plane = pl.BlockSpec((size_x, size_y), lambda i: (0, 0))
    x_shape = (levels // 5, 88, LANES)
    xa, xb = pl.pallas_call(
        functools.partial(pack_rows, size_x),
        grid=(steps,),
        in_specs=[low, high] * 4 + [plane],
        out_specs=[pl.BlockSpec((ZC // 5, 88, LANES), lambda i: (i, 0, 0))] * 2,
        out_shape=[sds(x_shape, F32)] * 2,
        name="pack_rows",
    )(
        u_wind, u_wind, v_wind, v_wind, pressure, pressure, w_wind, w_wind, vert_coef,
    )
    xa, xb, we_t, sn_t = lax.optimization_barrier(
        (
            xa,
            xb,
            jnp.transpose(we_slab, (0, 1, 3, 4, 2)),
            jnp.transpose(sn_slab, (0, 1, 3, 4, 2)),
        )
    )
    xa = swap(xa, "gx", False)
    xb = swap(xb, "gx", True)

    we_shape = (-(-3 * band // 4), 64, LANES)
    sn_shape = (3, -(-levels // SLOT), SUBL, LANES)
    pack_call = pl.pallas_call(
        functools.partial(pack_slabs, n_gx, n_gy),
        in_specs=[vmem] * 2,
        out_specs=[vmem] * (n_gx + n_gy),
        out_shape=[sds(we_shape, F32)] * n_gx + [sds(sn_shape, F32)] * n_gy,
        scratch_shapes=[
            pltpu.VMEM((2, LANES, LANES), F32),
            pltpu.VMEM((2, band, 3 * SUBL, LANES), F32),
        ],
        name="pack_slabs",
    )
    packed = pack_call(we_t, sn_t)
    we_all = to_ends(packed[0], packed[1:n_gx], "gx")
    sn_all = to_ends(packed[n_gx], packed[n_gx + 1 :], "gy")

    q_shape = (steps, 4 * ZC + 1, SUBL, LANES)
    c_shape = (steps, 6, SUBL, LANES)
    d_shape = (steps, 5, SUBL, LANES)
    blend_call = pl.pallas_call(
        functools.partial(blend_pack, n_gx, n_gy, m, xs, band),
        grid=(steps,),
        in_specs=[field] * 4
        + [plane] * 2
        + [fixed(we_shape)] * n_gx
        + [fixed(sn_shape)] * n_gy,
        out_specs=[field] * 3 + [lead(q_shape)] + [lead(c_shape)] * 2 + [lead(d_shape)] * 4,
        out_shape=[sds(pressure.shape, F32)] * 3
        + [sds(q_shape, F32)]
        + [sds(c_shape, F32)] * 2
        + [sds(d_shape, F32)] * 4,
        scratch_shapes=[
            pltpu.VMEM((3 * band, 64, LANES), F32),
            pltpu.VMEM((2, 5, 2, SUBL, LANES), F32),
        ],
        compiler_params=big,
        name="blend_pack",
    )
    ub, vb, pb, q, ca, cb, caa, cab, cba, cbb = blend_call(
        u_wind, v_wind, pressure, w_wind, vert_coef, relax_width, *we_all, *sn_all
    )
    qa = swap(q, "gy", False)
    qb = swap(q, "gy", True)
    ca = swap(ca, "gx", False)
    cb = swap(cb, "gx", True)
    caa = swap2(caa, False, False)
    cab = swap2(cab, False, True)
    cba = swap2(cba, True, False)
    cbb = swap2(cbb, True, True)

    whole = pl.BlockSpec(memory_space=pltpu.VMEM)
    tall = pltpu.VMEM((levels + 5, SUBL * (full + 1), LANES), F32)
    return pl.pallas_call(
        functools.partial(substeps, n_gx, n_gy),
        in_specs=[whole] * 15,
        out_specs=[whole] * 4,
        out_shape=[sds(pressure.shape, F32)] * 4,
        scratch_shapes=[
            pltpu.VMEM((levels + 5, SUBL * (full + 2), LANES), F32),
            pltpu.VMEM((levels + 5, SUBL, LANES), F32),
            tall, tall, tall, tall, tall,
            pltpu.VMEM((levels + 5, SUBL * (blocks + 2), LANES), F32),
            pltpu.VMEM((3, SUBL * (full + 1), LANES), F32),
        ],
        compiler_params=big,
        name="substeps",
    )(ub, vb, pb, w_wind, vert_coef, xa, xb, qa, qb, ca, cb, caa, cab, cba, cbb)


def solution(mesh):
    cell = P(None, "gx", "gy")
    placed = (
        cell, cell, cell, cell,
        P("gx", "gy"),
        P(None, None, None, None, ("gy", "gx")),
        P(None, None, None, None, ("gx", "gy")),
        P("gx", "gy"),
    )
    return jax.shard_map(
        per_device,
        mesh=mesh,
        in_specs=placed,
        out_specs=(cell, cell, cell, cell),
        check_vma=False,
    )
```

```python
import functools
import jax
import jax.numpy as jnp
from jax import lax
from jax.experimental import pallas as pl
from jax.experimental.pallas import tpu as pltpu
from jax.sharding import PartitionSpec as P

SUBSTEPS = 6
ACCEL = 0.3
SPREAD = 0.3
BUOYANCY = 0.5
UNIT = 1.0 / ACCEL
DEEP = 6
GROUP = 2 * DEEP
ZC = 20
SUBL = 8
LANES = 128
F32 = jnp.float32


def lane_ids():
    return lax.broadcasted_iota(jnp.int32, (SUBL, LANES), 1)


def sub_ids():
    return lax.broadcasted_iota(jnp.int32, (SUBL, LANES), 0)


def lroll(x, shift):
    if isinstance(shift, int):
        shift = shift % LANES
        if shift == 0:
            return x
    return pltpu.roll(x, shift, 1)


def sroll(x, shift):
    return pltpu.roll(x, shift % SUBL, 0)


SLOT = 25


def pack_slabs(n_gx, n_gy, we, sn, *refs):
    we_own, sn_own = refs[0], refs[n_gx]
    we_out, sn_out = refs[1:n_gx], refs[n_gx + 1 : n_gx + n_gy]
    tile, flat = refs[n_gx + n_gy :]
    gx = lax.axis_index("gx")
    gy = lax.axis_index("gy")
    band, m, levels = we.shape[2:]
    xs = sn.shape[3]
    groups = we_own.shape[0]
    slots = sn_own.shape[1]
    tile[...] = jnp.zeros_like(tile)
    flat[...] = jnp.zeros_like(flat)
    for g in range(groups):
        for side in range(2):
            for c in range(4):
                fd = 4 * g + c
                if fd < 3 * band:
                    tile[side, m * c : m * (c + 1), 0:levels] = we[side, fd // band, fd % band]
        west = tile[0].T[0 : we_own.shape[1]]
        east = tile[1].T[0 : we_own.shape[1]]
        we_own[g] = jnp.where(gx == 0, west, east)
        for k, ref in enumerate(we_out):
            ref[g] = jnp.where(gx == k + 1, west, east)
    level = lax.broadcasted_iota(jnp.int32, (LANES, LANES), 0)
    lane = lax.broadcasted_iota(jnp.int32, (LANES, LANES), 1)
    for f in range(3):
        for side in range(2):
            for d in range(band):
                for rep in range(SUBL // xs):
                    lo = SUBL * f + xs * rep
                    flat[side, d, lo : lo + xs, 0:levels] = sn[side, f, d]
    for t in range(slots):
        vals = []
        for side in range(2):
            acc = jnp.zeros((3 * SUBL, LANES), F32)
            for d in range(band):
                at = d if side == 0 else band - 1 - d
                put = (lane == band * (level - SLOT * t) + at) & (level >= SLOT * t)
                put = put & (level < SLOT * (t + 1))
                acc = acc + jnp.dot(
                    flat[side, d],
                    put.astype(F32),
                    precision=lax.Precision.HIGHEST,
                    preferred_element_type=F32,
                )
            vals.append(acc)
        for f in range(3):
            south = vals[0][SUBL * f : SUBL * (f + 1)]
            north = vals[1][SUBL * f : SUBL * (f + 1)]
            sn_own[f, t] = jnp.where(gy == 0, south, north)
            for k, ref in enumerate(sn_out):
                ref[f, t] = jnp.where(gy == k + 1, south, north)


def pack_rows(size_x, u0, u7, v0, v7, p0, p7, w0, w7, r, xa, xb):
    even = (lax.axis_index("gx") % 2) == 0
    lane = lane_ids()
    sub = sub_ids()

    def body(h, carry):
        for c5 in range(5):
            z = h * 5 + c5
            ut, ub, vt, vb = u7[z], u0[z], v7[z], v0[z]
            e7 = UNIT * ((ut - sroll(ut, 1)) + (vt - jnp.where(lane == 0, 0.0, lroll(vt, 1))))
            up0 = jnp.where(sub == 0, 0.0, sroll(ub, 1))
            e0 = UNIT * ((ub - up0) + (vb - jnp.where(lane == 0, 0.0, lroll(vb, 1))))
            ea = jnp.where(sub < 2, sroll(e7, -3), p7[z])
            eb = jnp.where(sub < 3, sroll(e7, -5), w7[z])
            wa = jnp.where(sub < 6, p0[z], sroll(e0, 6))
            wb = jnp.where(sub < 5, w0[z], sroll(e0, 3))
            at = 2 * SUBL * c5
            xa[h, at : at + SUBL, :] = jnp.where(even, ea, wa)
            xa[h, at + SUBL : at + 2 * SUBL, :] = jnp.where(even, eb, wb)
            xb[h, at : at + SUBL, :] = jnp.where(even, wa, ea)
            xb[h, at + SUBL : at + 2 * SUBL, :] = jnp.where(even, wb, eb)
            last = ut[SUBL - 1 : SUBL, :]
            xa[h, 80 + c5 : 81 + c5, :] = last
            xb[h, 80 + c5 : 81 + c5, :] = last
        return carry

    lax.fori_loop(0, xa.shape[0], body, 0)
    east_r = r[size_x - 5 : size_x, :]
    west_r = r[0:5, :]
    ra = jnp.where(even, east_r, west_r)
    rb = jnp.where(even, west_r, east_r)
    for ref, val in ((xa, ra), (xb, rb)):
        ref[0, 85:88, :] = val[0:3]
        ref[1, 85:87, :] = val[3:5]
        ref[1, 87:88, :] = val[4:5]
        ref[2, 85:88, :] = val[0:3]
        ref[3, 85:88, :] = val[0:3]


def blend_pack(n_gx, n_gy, m, xs, band, *refs):
    u, v, p, w, r, rate = refs[:6]
    refs = refs[6:]
    we_own, sn_own = refs[0], refs[n_gx]
    we_in = refs[1:n_gx]
    sn_in = refs[n_gx + 1 : n_gx + n_gy]
    ub, vb, pb, q, ca, cb, daa, dab, dba, dbb, rows_we, corners = refs[n_gx + n_gy :]
    gx = lax.axis_index("gx")
    gy = lax.axis_index("gy")
    chunk = pl.program_id(0)
    size_x = u.shape[1]
    blocks = size_x // SUBL
    outs = (ub, vb, pb)
    for src, dst in zip((u, v, p), outs):
        dst[...] = src[...]
    lane = lane_ids()
    sub = sub_ids()

    def band_blend(pieces, row_of):
        tall_lane = lax.broadcasted_iota(jnp.int32, rows_we.shape[1:], 1)

        @pl.when(chunk == 0)
        def _():
            for fd in range(3 * band):
                g, c = divmod(fd, 4)
                val = None
                for s, piece in enumerate(pieces):
                    moved = lroll(piece[g], m * (s - c))
                    if val is None:
                        val = moved
                    else:
                        val = jnp.where(tall_lane >= m * s, moved, val)
                rows_we[fd] = val

        wts = []
        for d in range(band):
            rt = rate[row_of(d) : row_of(d) + 1, :].astype(F32)
            wts.append(jnp.maximum(rt - float(d), 0.0) / rt)

        def body(h, carry):
            for i in range(5):
                z = h * 5 + i
                for f in range(3):
                    for d in range(band):
                        at = slice(row_of(d), row_of(d) + 1)
                        val = rows_we[f * band + d, pl.ds(chunk * ZC + z, 1), :]
                        old = outs[f][z, at, :]
                        outs[f][z, at, :] = old + wts[d] * (val - old)
            return carry

        lax.fori_loop(0, ZC // 5, body, 0)

    @pl.when(gx == 0)
    def _():
        band_blend([we_own] + [we_in[s - 1] for s in range(1, n_gx)], lambda d: d)

    @pl.when(gx == n_gx - 1)
    def _():
        band_blend(
            [we_in[n_gx - 2 - s] for s in range(n_gx - 1)] + [we_own],
            lambda d: size_x - 1 - d,
        )

    per = SUBL // xs

    def side_blend(pieces, first, dist):
        wts = []
        for b in range(blocks):
            rt = rate[SUBL * b : SUBL * (b + 1), :].astype(F32)
            wts.append(jnp.maximum(rt - dist, 0.0) / rt)

        def body(h, carry):
            for z in [h * 5 + i for i in range(5)]:
                t, c = (chunk * ZC + z) // SLOT, (chunk * ZC + z) % SLOT
                shift = jnp.mod(first - band * c + LANES, LANES)
                for f in range(3):
                    for b in range(blocks):
                        val = pieces[b * per][f, t]
                        for s in range(1, per):
                            val = jnp.where(sub // xs == s, pieces[b * per + s][f, t], val)
                        val = pltpu.roll(val, shift, 1)
                        old = outs[f][z, SUBL * b : SUBL * (b + 1), :]
                        outs[f][z, SUBL * b : SUBL * (b + 1), :] = old + wts[b] * (val - old)
            return carry

        lax.fori_loop(0, ZC // 5, body, 0)

    @pl.when(gy == 0)
    def _():
        side_blend([sn_own] + [sn_in[s - 1] for s in range(1, n_gy)], 0, lane.astype(F32))

    @pl.when(gy == n_gy - 1)
    def _():
        side_blend(
            [sn_in[n_gy - 2 - s] for s in range(n_gy - 1)] + [sn_own],
            LANES - band,
            (LANES - 1 - lane).astype(F32),
        )

    def strip_of(blocks_of):
        acc = jnp.zeros((SUBL, LANES), F32)
        for b in range(blocks):
            lo = GROUP * (b + 1)
            moved = lroll(blocks_of(b), lo + DEEP)
            acc = jnp.where((lane >= lo) & (lane < lo + GROUP), moved, acc)
        return acc

    x_even = (gx % 2) == 0
    y_even = (gy % 2) == 0
    bases = [
        jnp.where(x_even, LANES - GROUP * blocks, LANES - GROUP),
        jnp.where(x_even, LANES - GROUP, LANES - GROUP * blocks),
    ]

    def body(t, carry):
        for f, src in enumerate((ub, vb, pb, w)):
            strips = []
            for c in range(10):
                z = t * 10 + c
                strip = strip_of(lambda b: src[z, SUBL * b : SUBL * (b + 1), :])
                q[0, f * ZC + z] = strip
                strips.append(strip)
            for side in range(2):
                acc = jnp.zeros((SUBL, LANES), F32)
                for c in range(10):
                    moved = pltpu.roll(strips[c], jnp.mod(bases[side] + GROUP * c, LANES), 1)
                    here = (lane >= GROUP * c) & (lane < GROUP * (c + 1))
                    acc = jnp.where(here, moved, acc)
                corners[side, f, t] = acc
        return carry

    lax.fori_loop(0, ZC // 10, body, 0)
    strip = strip_of(lambda b: r[SUBL * b : SUBL * (b + 1), :])
    q[0, 4 * ZC] = strip
    low_half = lane % GROUP < DEEP
    for side, near, diag in ((0, ca, (daa, dab)), (1, cb, (dba, dbb))):
        corners[side, 4, 0] = pltpu.roll(strip, bases[side], 1)
        corners[side, 4, 1] = corners[side, 4, 0]
        for f in range(3):
            for t in range(2):
                near[0, 2 * f + t] = corners[side, f, t]
        for way, out in enumerate(diag):
            high = y_even if way == 0 else jnp.logical_not(y_even)
            first = jnp.where(high, 0, LANES - DEEP)
            second = jnp.where(high, DEEP, 0)
            for f in range(5):
                a = pltpu.roll(corners[side, f, 0], first, 1)
                b = pltpu.roll(corners[side, f, 1], second, 1)
                out[0, f] = jnp.where(low_half, a, b)


def prepare(u, v, f_out):
    blocks = u.shape[1] // SUBL
    lane = lane_ids()
    sub = sub_ids()

    def body(i, carry):
        for z in (2 * i, 2 * i + 1):
            for b in range(blocks):
                rows = slice(SUBL * b, SUBL * (b + 1))
                uu, vv = u[z, rows, :], v[z, rows, :]
                if b == 0:
                    up = jnp.where(sub == 0, 0.0, sroll(uu, 1))
                else:
                    up = u[z, SUBL * b - 1 : SUBL * (b + 1) - 1, :]
                left = jnp.where(lane == 0, 0.0, lroll(vv, 1))
                f_out[z, rows, :] = UNIT * ((uu - up) + (vv - left))
        return carry

    lax.fori_loop(0, u.shape[0] // 2, body, 0)


def substeps(n_gx, n_gy, *refs):
    (ub_in, vb_in, pb_in, f_in, w_in) = refs[:5]
    (r, xa, xb, qa, qb, qo, ca, cb, caa, cab, cba, cbb) = refs[5:17]
    outs = refs[17:21]
    (PM, FM, WM, GM, QM, LM, SM, KM, ub, vb, u_out, v_out, w_out, p_out, sems) = refs[21:]
    levels, size_x = ub.shape[0], ub.shape[1]
    main = pl.ds(SUBL, size_x)
    loads = []
    for n, (src, dst) in enumerate(
        (
            (pb_in, PM.at[pl.ds(0, levels), pl.ds(2 * SUBL, size_x)]),
            (f_in, FM.at[pl.ds(0, levels), main]),
            (ub_in, ub),
            (w_in, WM.at[pl.ds(1, levels), main]),
            (vb_in, vb),
        )
    ):
        copy = pltpu.make_async_copy(src, dst, sems.at[n])
        copy.start()
        loads.append(copy)
    blocks = size_x // SUBL
    full = blocks + 2
    every = range(full + 1)
    gx = lax.axis_index("gx")
    gy = lax.axis_index("gy")
    x_even = (gx % 2) == 0
    y_even = (gy % 2) == 0
    is_w, is_e = gx == 0, gx == n_gx - 1
    is_s, is_n = gy == 0, gy == n_gy - 1
    lane = lane_ids()
    sub = sub_ids()
    within = lane % GROUP
    block_of = lane // GROUP
    low_half = within < DEEP
    rim_lo, rim_hi = within == DEEP - 1, within == DEEP
    zero = jnp.zeros((SUBL, LANES), F32)
    rows = [slice(SUBL * b, SUBL * (b + 1)) for b in range(full + 2)]
    COEF, RINV, STEP = 0, 1, 2

    def strip_from(mine, cw, ce, spot):
        west = pltpu.roll(cw, jnp.mod(LANES - GROUP * spot, LANES), 1)
        east = pltpu.roll(ce, jnp.mod(LANES + GROUP * (full - 1) - GROUP * spot, LANES), 1)
        got = jnp.where(block_of == 0, west, mine)
        return jnp.where(block_of == full - 1, east, got)

    def four(k, i, late):
        aa, ab, ba, bb = caa[k, i], cab[k, i], cba[k, i], cbb[k, i]
        back = jnp.where(late, LANES - DEEP, 0)
        ahead = jnp.where(late, 0, DEEP)
        pairs = []
        for sa, sb in ((aa, ab), (ba, bb)):
            south, north = jnp.where(y_even, sb, sa), jnp.where(y_even, sa, sb)
            south, north = pltpu.roll(south, back, 1), pltpu.roll(north, ahead, 1)
            pairs.append(jnp.where(low_half, south, north))
        a, b = pairs
        return jnp.where(x_even, b, a), jnp.where(x_even, a, b)

    def strip_at(k, iq, corners, spot):
        a, b = qa[k, iq], qb[k, iq]
        mine = jnp.where(low_half == y_even, b, a)
        return strip_from(mine, corners[0], corners[1], spot)

    def strip_rows(s):
        up = sroll(s, 1)
        up = jnp.where(sub == 0, lroll(up, GROUP), up)
        dn = sroll(s, -1)
        dn = jnp.where(sub == SUBL - 1, lroll(dn, -GROUP), dn)
        return up, dn

    row_first = is_w & (block_of == 1) & (sub == 0)
    row_last = is_e & (block_of == full - 2) & (sub == SUBL - 1)
    lane0, lane_end = lane == 0, lane == LANES - 1
    lane0_in, lane0_rim = lane0 & jnp.logical_not(is_s), lane0 & is_s
    strip_zero = is_n & rim_hi
    fix_w, fix_e = is_w & (sub == SUBL - 1), is_e & (sub == 0)

    def put_pressure(z, tiles):
        tiles = list(tiles)
        tiles[0] = jnp.where(fix_w, sroll(tiles[1], -1), tiles[0])
        tiles[full - 1] = jnp.where(fix_e, 0.0, tiles[full - 1])
        ps = jnp.where(strip_zero, 0.0, tiles[full])
        PM[z, rows[full + 1], :] = ps
        rims = zero
        for b in range(full):
            p0 = tiles[b]
            PM[z, rows[b + 1], :] = p0
            lo = GROUP * b + DEEP
            rims = jnp.where((lane == lo) | (lane == lo - 1), lroll(p0, lo), rims)
            LM[z, rows[b], :] = lroll(ps, -lo)
        s_lf = lroll(jnp.where(rim_lo, rims, ps), 1)
        s_rt = lroll(jnp.where(rim_hi, rims, ps), -1)
        up, dn = strip_rows(ps)
        up = jnp.where(row_first, ps, up)
        dn = jnp.where(row_last, 0.0, dn)
        LM[z, rows[full], :] = (s_lf + s_rt) + (up + dn)

    west_x = lambda h, lo, hi: jnp.where(x_even, xb[h, lo:hi, :], xa[h, lo:hi, :])
    east_x = lambda h, lo, hi: jnp.where(x_even, xa[h, lo:hi, :], xb[h, lo:hi, :])
    KM[COEF] = jnp.ones(KM.shape[1:], F32)
    KM[COEF, SUBL : SUBL * (blocks + 1), :] = r[...]
    KM[COEF, 3:6, :] = west_x(0, 85, 88)
    KM[COEF, 6:8, :] = west_x(1, 85, 87)
    lo = SUBL * (full - 1)
    KM[COEF, lo : lo + 3, :] = east_x(0, 85, 88)
    KM[COEF, lo + 3 : lo + 5, :] = east_x(1, 85, 87)
    KM[COEF, rows[full], :] = strip_at(0, 4 * ZC, four(0, 4, False), 0)
    kappas, rhos = [], []
    for b in every:
        c = KM[COEF, rows[b], :]
        c = jnp.where(c > 0.0, c, 1.0)
        KM[RINV, rows[b], :] = 1.0 / c
        KM[STEP, rows[b], :] = BUOYANCY / c
        k = 2.0 * c / ((1.0 + 2.0 * c) + jnp.sqrt(1.0 + 4.0 * c))
        kappas.append(k)
        rhos.append(k * k)

    def factor_body(z, carry):
        powers, lows = [], []
        for b in every:
            powers.append(carry[0][b] * rhos[b])
            lows.append(1.0 - powers[b])
            GM[z + 1, rows[b], :] = kappas[b] * (carry[1][b] / lows[b])
        return tuple(powers), tuple(lows)

    lax.fori_loop(0, levels, factor_body, (tuple(rhos), tuple(1.0 - x for x in rhos)))
    wide = jnp.zeros(FM.shape[1:], F32)
    GM[0] = wide
    WM[0] = wide
    for z in range(levels, FM.shape[0]):
        FM[z] = wide
        LM[z] = wide
        PM[z] = wide
        SM[z] = wide

    s5 = ZC // 5

    def patch(near, side, spot, p_old, f_old):
        shift = jnp.mod(LANES - GROUP * spot - DEEP, LANES)
        uu, vv, pp = [pltpu.roll(near[f][side], shift, 1) for f in range(3)]
        up = sroll(uu, 1)
        if side == 1:
            up = jnp.where(sub == 0, 0.0, up)
        f_new = UNIT * ((uu - up) + (vv - jnp.where(lane0, 0.0, lroll(vv, 1))))
        mine_s, mine_n = is_s & (lane < DEEP), is_n & (lane > LANES - DEEP)
        here = mine_s | mine_n
        return jnp.where(here, pp, p_old), jnp.where(here, f_new, f_old), (here, uu)

    def unpack(patched, h, carry):
        k, hh = h // s5, h % s5
        late = hh // 2
        corners = [four(k, f, late == 1) for f in range(4)]
        near = []
        for f in range(3):
            a, b = ca[k, 2 * f + late], cb[k, 2 * f + late]
            near.append((jnp.where(x_even, b, a), jnp.where(x_even, a, b)))
        v_w, v_e = near[1]
        for c5 in range(5):
            z, zz = h * 5 + c5, hh * 5 + c5
            spot = (hh % 2) * 5 + c5
            us, vs, ps, ws = [strip_at(k, f * ZC + zz, corners[f], spot) for f in range(4)]
            at = 2 * SUBL * c5
            xa_a, xa_b = xa[h, at : at + SUBL, :], xa[h, at + SUBL : at + 2 * SUBL, :]
            xb_a, xb_b = xb[h, at : at + SUBL, :], xb[h, at + SUBL : at + 2 * SUBL, :]
            wa, wb = jnp.where(x_even, xb_a, xa_a), jnp.where(x_even, xb_b, xa_b)
            ea, eb = jnp.where(x_even, xa_a, xb_a), jnp.where(x_even, xa_b, xb_b)
            f_west = jnp.where(sub < 5, sroll(wa, 3), sroll(wb, 5))
            f_east = jnp.where(sub < 2, sroll(ea, 2), sroll(eb, -3))
            u_side = None
            if patched:
                wa, f_west, u_side = patch(near, 0, spot, wa, f_west)
                ea, f_east, _ = patch(near, 1, spot, ea, f_east)
            u_row = jnp.where(x_even, xb[h, 80 + c5 : 81 + c5, :], xa[h, 80 + c5 : 81 + c5, :])
            if u_side is not None:
                here, uu = u_side
                u_row = jnp.where(here, sroll(uu, 1), u_row)
            u_row = jnp.where(is_w, 0.0, u_row)
            v_left = jnp.where(block_of == 0, zero, qo[k, ZC + zz])
            far = strip_from(v_left, v_w, v_e, spot)
            v_left = lroll(jnp.where(rim_lo, far, vs), 1)
            u_up, _ = strip_rows(us)
            FM[z, rows[full], :] = UNIT * ((us - u_up) + (vs - v_left))
            WM[z + 1, rows[full], :] = ws
            WM[z + 1, rows[0], :] = wb
            WM[z + 1, rows[full - 1], :] = eb
            ps = jnp.where(strip_zero, 0.0, ps)
            wa = jnp.where(fix_w, sroll(PM[z, rows[2], :], -1), wa)
            ea = jnp.where(fix_e, 0.0, ea)
            PM[z, rows[0], :] = zero
            PM[z, rows[1], :] = wa
            PM[z, rows[full], :] = ea
            PM[z, rows[full + 1], :] = ps
            rims = qo[k, 2 * ZC + zz]
            lo = GROUP * (full - 1) + DEEP
            rims = jnp.where(block_of == 0, lroll(wa, DEEP), rims)
            rims = jnp.where(block_of == full - 1, lroll(ea, lo), rims)
            s_lf = lroll(jnp.where(rim_lo, rims, ps), 1)
            s_rt = lroll(jnp.where(rim_hi, rims, ps), -1)
            up, dn = strip_rows(ps)
            up = jnp.where(row_first, ps, up)
            dn = jnp.where(row_last, 0.0, dn)
            LM[z, rows[full], :] = (s_lf + s_rt) + (up + dn)
            for b in range(full):
                lo = GROUP * b + DEEP
                LM[z, rows[b], :] = lroll(ps, -lo)
                less = jnp.where(lane0, lroll(vs, 1 - lo), 0.0)
                if b == 0:
                    f = f_west
                elif b == full - 1:
                    f = f_east
                    u63 = sroll(ub[z, rows[blocks - 1], :], 1)
                    less = less + jnp.where(sub == 0, u63, 0.0)
                else:
                    f = FM[z, rows[b], :]
                    if b == 1:
                        less = less + jnp.where(sub == 0, u_row, 0.0)
                FM[z, rows[b], :] = f - UNIT * less
            SM[z] = wide
        return carry

    rim = is_s | is_n
    for copy in loads[:3]:
        copy.wait()

    @pl.when(rim)
    def _():
        lax.fori_loop(0, levels // 5, functools.partial(unpack, True), 0)

    @pl.when(jnp.logical_not(rim))
    def _():
        lax.fori_loop(0, levels // 5, functools.partial(unpack, False), 0)

    coef_step = ACCEL * SPREAD
    inner = range(1, full - 1)

    def section(z, last):
        for b in every:
            p0 = PM[z, rows[b + 1], :]
            if b >= 1:
                SM[z, rows[b - 1], :] += p0
            if last and b not in inner:
                continue
            around = LM[z, rows[b], :]
            if b < full:
                lf = lroll(jnp.where(lane_end, around, p0), 1)
                lf = jnp.where(lane0_rim, p0, lf)
                rt = lroll(jnp.where(lane0, around, p0), -1)
                up = PM[z, SUBL * (b + 1) - 1 : SUBL * (b + 2) - 1, :]
                dn = PM[z, SUBL * (b + 1) + 1 : SUBL * (b + 2) + 1, :]
                around = (lf + rt) + (up + dn)
            f = FM[z, rows[b], :] + (4.0 * p0 - around)
            if not last:
                FM[z, rows[b], :] = f
            QM[z, rows[b], :] = p0 - coef_step * f

    def run_step(last):
        active = inner if last else every
        for z in range(5):
            section(z, last)

        def forward(i, carry):
            d_prev = dict(zip(active, carry))
            for c in range(4):
                section(4 * i + 5 + c, last)
            for c in range(4):
                z = 4 * i + c
                for b in active:
                    change = QM[z, rows[b], :] - QM[z + 1, rows[b], :]
                    rhs = WM[z + 1, rows[b], :] * KM[RINV, rows[b], :] + KM[STEP, rows[b], :] * change
                    d = GM[z + 1, rows[b], :] * (rhs + d_prev[b])
                    WM[z + 1, rows[b], :] = d
                    d_prev[b] = d
            return tuple(d_prev[b] for b in active)

        tops = lax.fori_loop(0, levels // 4, forward, tuple(zero for _ in active))

        def backward(i, above):
            above = dict(zip(active, above))
            for c in range(4):
                z = levels - 1 - (4 * i + c)
                tiles = {}
                below = {}
                for b in active:
                    ww = WM[z, rows[b], :] + GM[z, rows[b], :] * above[b]
                    tiles[b] = QM[z, rows[b], :] - BUOYANCY * (above[b] - ww)
                    if not last:
                        WM[z, rows[b], :] = ww
                    below[b] = ww
                if last:
                    ss = SM[z, rows[blocks + 1], :]
                    for b in active:
                        m = rows[b - 1]
                        w_out[z, m, :] = above[b]
                        p_out[z, m, :] = tiles[b]
                        s0 = SM[z, m, :]
                        dn = SM[z, SUBL * (b - 1) + 1 : SUBL * b + 1, :]
                        rt = jnp.where(
                            lane_end, lroll(ss, -1 - (GROUP * b + DEEP)), lroll(s0, -1)
                        )
                        u_out[z, m, :] = ub[z, m, :] - ACCEL * (dn - s0)
                        v_out[z, m, :] = vb[z, m, :] - ACCEL * (rt - s0)
                else:
                    put_pressure(z, [tiles[b] for b in every])
                above = below
            if last:
                part = pl.ds(levels - 4 - 4 * i, 4)
                for n, (src, dst) in enumerate(zip((u_out, v_out, w_out, p_out), outs)):
                    pltpu.make_async_copy(src.at[part], dst.at[part], sems.at[5 + n]).start()
            return tuple(above[b] for b in active)

        lax.fori_loop(0, levels // 4, backward, tops)

    loads[3].wait()

    def step(_, carry):
        run_step(False)
        return carry

    lax.fori_loop(0, SUBSTEPS - 1, step, 0)
    loads[4].wait()
    run_step(True)
    for n, (src, dst) in enumerate(zip((u_out, v_out, w_out, p_out), outs)):
        pltpu.make_async_copy(src, dst, sems.at[5 + n]).wait()


def swap(block, axis, second):
    n = lax.axis_size(axis)
    return lax.ppermute(block, axis, pairing(n, second))


def pairing(n, second):
    lo = 1 if second else 0
    pairs = []
    for i in range(lo, n - 1, 2):
        pairs += [(i, i + 1), (i + 1, i)]
    return pairs


def swap2(block, second_x, second_y):
    nx, ny = lax.axis_size("gx"), lax.axis_size("gy")
    pairs = []
    for a, b in pairing(nx, second_x):
        for c, d in pairing(ny, second_y):
            pairs.append((a * ny + c, b * ny + d))
    return lax.ppermute(block, ("gx", "gy"), pairs)


def to_ends(own, blocks, axis):
    n = lax.axis_size(axis)
    got = [own]
    for k, block in enumerate(blocks, 1):
        got.append(lax.ppermute(block, axis, [(k, 0), (n - 1 - k, n - 1)]))
    return got


def per_device(u_wind, v_wind, w_wind, pressure, vert_coef, we_slab, sn_slab, relax_width):
    n_gx, n_gy = lax.axis_size("gx"), lax.axis_size("gy")
    levels, size_x, size_y = pressure.shape
    blocks = size_x // SUBL
    band, m = we_slab.shape[3], we_slab.shape[4]
    xs = sn_slab.shape[4]
    steps = levels // ZC
    sds = jax.ShapeDtypeStruct
    big = pltpu.CompilerParams(vmem_limit_bytes=60 * 1024 * 1024)
    vmem = pl.BlockSpec(memory_space=pltpu.VMEM)

    lead = lambda shape: pl.BlockSpec((1,) + shape[1:], lambda i: (i,) + (0,) * (len(shape) - 1))
    fixed = lambda shape: pl.BlockSpec(shape, lambda i: (0,) * len(shape))
    field = pl.BlockSpec((ZC, size_x, size_y), lambda i: (i, 0, 0))
    low = pl.BlockSpec((ZC, SUBL, size_y), lambda i: (i, 0, 0))
    high = pl.BlockSpec((ZC, SUBL, size_y), lambda i: (i, blocks - 1, 0))
    plane = pl.BlockSpec((size_x, size_y), lambda i: (0, 0))
    x_shape = (levels // 5, 88, LANES)
    rows_call = pl.pallas_call(
        functools.partial(pack_rows, size_x),
        grid=(steps,),
        in_specs=[low, high] * 4 + [plane],
        out_specs=[pl.BlockSpec((ZC // 5, 88, LANES), lambda i: (i, 0, 0))] * 2,
        out_shape=[sds(x_shape, F32)] * 2,
        name="pack_rows",
    )
    xa, xb = rows_call(
        u_wind, u_wind, v_wind, v_wind, pressure, pressure, w_wind, w_wind, vert_coef,
    )
    xa = swap(xa, "gx", False)
    xb = swap(xb, "gx", True)

    we_t = jnp.transpose(we_slab, (0, 1, 3, 4, 2))
    sn_t = jnp.transpose(sn_slab, (0, 1, 3, 4, 2))
    we_shape = (-(-3 * band // 4), 64, LANES)
    sn_shape = (3, -(-levels // SLOT), SUBL, LANES)
    pack_call = pl.pallas_call(
        functools.partial(pack_slabs, n_gx, n_gy),
        in_specs=[vmem] * 2,
        out_specs=[vmem] * (n_gx + n_gy),
        out_shape=[sds(we_shape, F32)] * n_gx + [sds(sn_shape, F32)] * n_gy,
        scratch_shapes=[
            pltpu.VMEM((2, LANES, LANES), F32),
            pltpu.VMEM((2, band, 3 * SUBL, LANES), F32),
        ],
        name="pack_slabs",
    )
    packed = pack_call(we_t, sn_t)
    we_all = to_ends(packed[0], packed[1:n_gx], "gx")
    sn_all = to_ends(packed[n_gx], packed[n_gx + 1 :], "gy")

    q_shape = (steps, 4 * ZC + 1, SUBL, LANES)
    c_shape = (steps, 6, SUBL, LANES)
    d_shape = (steps, 5, SUBL, LANES)
    blend_call = pl.pallas_call(
        functools.partial(blend_pack, n_gx, n_gy, m, xs, band),
        grid=(steps,),
        in_specs=[field] * 4
        + [plane] * 2
        + [fixed(we_shape)] * n_gx
        + [fixed(sn_shape)] * n_gy,
        out_specs=[field] * 3 + [lead(q_shape)] + [lead(c_shape)] * 2 + [lead(d_shape)] * 4,
        out_shape=[sds(pressure.shape, F32)] * 3
        + [sds(q_shape, F32)]
        + [sds(c_shape, F32)] * 2
        + [sds(d_shape, F32)] * 4,
        scratch_shapes=[
            pltpu.VMEM((3 * band, 64, LANES), F32),
            pltpu.VMEM((2, 5, 2, SUBL, LANES), F32),
        ],
        compiler_params=big,
        name="blend_pack",
    )
    ub, vb, pb, q, ca, cb, caa, cab, cba, cbb = blend_call(
        u_wind, v_wind, pressure, w_wind, vert_coef, relax_width, *we_all, *sn_all
    )
    qa = swap(q, "gy", False)
    qb = swap(q, "gy", True)
    ca = swap(ca, "gx", False)
    cb = swap(cb, "gx", True)
    caa = swap2(caa, False, False)
    cab = swap2(cab, False, True)
    cba = swap2(cba, True, False)
    cbb = swap2(cbb, True, True)
    prep_call = pl.pallas_call(
        prepare,
        grid=(steps,),
        in_specs=[field] * 2,
        out_specs=field,
        out_shape=sds(pressure.shape, F32),
        compiler_params=big,
        name="prepare",
    )
    f_main = prep_call(ub, vb)

    whole = pl.BlockSpec(memory_space=pltpu.VMEM)
    tall = pltpu.VMEM((levels + 5, 96, LANES), F32)
    own = pltpu.VMEM(pressure.shape, F32)
    far = pl.BlockSpec(memory_space=pl.ANY)
    return pl.pallas_call(
        functools.partial(substeps, n_gx, n_gy),
        in_specs=[far] * 5 + [whole] * 12,
        out_specs=[far] * 4,
        out_shape=[sds(pressure.shape, F32)] * 4,
        scratch_shapes=[tall] * 7
        + [pltpu.VMEM((3, 96, LANES), F32)]
        + [own] * 6
        + [pltpu.SemaphoreType.DMA((9,))],
        compiler_params=big,
        name="substeps",
    )(
        ub, vb, pb, f_main, w_wind,
        vert_coef, xa, xb, qa, qb, q, ca, cb, caa, cab, cba, cbb,
    )


def solution(mesh):
    cell = P(None, "gx", "gy")
    placed = (
        cell, cell, cell, cell,
        P("gx", "gy"),
        P(None, None, None, None, ("gy", "gx")),
        P(None, None, None, None, ("gx", "gy")),
        P("gx", "gy"),
    )
    return jax.shard_map(
        per_device,
        mesh=mesh,
        in_specs=placed,
        out_specs=(cell, cell, cell, cell),
        check_vma=False,
    )
```

```python
import functools
import jax
import jax.numpy as jnp
from jax import lax
from jax.experimental import pallas as pl
from jax.experimental.pallas import tpu as pltpu
from jax.sharding import PartitionSpec as P

SUBSTEPS = 6
ACCEL = 0.3
SPREAD = 0.3
BUOYANCY = 0.5
UNIT = 1.0 / ACCEL
DEEP = 6
GROUP = 2 * DEEP
ZC = 20
SUBL = 8
LANES = 128
F32 = jnp.float32
BF16 = jnp.bfloat16


def lane_ids():
    return lax.broadcasted_iota(jnp.int32, (SUBL, LANES), 1)


def sub_ids():
    return lax.broadcasted_iota(jnp.int32, (SUBL, LANES), 0)


def lroll(x, shift):
    if isinstance(shift, int):
        shift = shift % LANES
        if shift == 0:
            return x
    return pltpu.roll(x, shift, 1)


def sroll(x, shift):
    return pltpu.roll(x, shift % SUBL, 0)


FORE = 10
BACK = 6
SLOT = 25


def pack_slabs(n_gx, n_gy, we, sn, *refs):
    we_own, sn_own = refs[0], refs[n_gx]
    we_out, sn_out = refs[1:n_gx], refs[n_gx + 1 : n_gx + n_gy]
    tile, flat = refs[n_gx + n_gy :]
    gx = lax.axis_index("gx")
    gy = lax.axis_index("gy")
    band, m, levels = we.shape[2:]
    xs = sn.shape[3]
    groups = we_own.shape[0]
    slots = sn_own.shape[1]
    tile[...] = jnp.zeros_like(tile)
    flat[...] = jnp.zeros_like(flat)
    for g in range(groups):
        for side in range(2):
            for c in range(4):
                fd = 4 * g + c
                if fd < 3 * band:
                    tile[side, m * c : m * (c + 1), 0:levels] = we[side, fd // band, fd % band]
        west = tile[0].T[0 : we_own.shape[1]]
        east = tile[1].T[0 : we_own.shape[1]]
        we_own[g] = jnp.where(gx == 0, west, east)
        for k, ref in enumerate(we_out):
            ref[g] = jnp.where(gx == k + 1, west, east)
    level = lax.broadcasted_iota(jnp.int32, (LANES, LANES), 0)
    lane = lax.broadcasted_iota(jnp.int32, (LANES, LANES), 1)
    for f in range(3):
        for side in range(2):
            for d in range(band):
                for rep in range(SUBL // xs):
                    lo = SUBL * f + xs * rep
                    flat[side, d, lo : lo + xs, 0:levels] = sn[side, f, d]
    for t in range(slots):
        vals = []
        for side in range(2):
            acc = jnp.zeros((3 * SUBL, LANES), F32)
            for d in range(band):
                at = d if side == 0 else band - 1 - d
                put = (lane == band * (level - SLOT * t) + at) & (level >= SLOT * t)
                put = put & (level < SLOT * (t + 1))
                acc = acc + jnp.dot(
                    flat[side, d],
                    put.astype(F32),
                    precision=lax.Precision.HIGHEST,
                    preferred_element_type=F32,
                )
            vals.append(acc)
        for f in range(3):
            south = vals[0][SUBL * f : SUBL * (f + 1)]
            north = vals[1][SUBL * f : SUBL * (f + 1)]
            sn_own[f, t] = jnp.where(gy == 0, south, north)
            for k, ref in enumerate(sn_out):
                ref[f, t] = jnp.where(gy == k + 1, south, north)


def pack_rows(size_x, u0, u7, v0, v7, p0, p7, w0, w7, r, xa, xb):
    even = (lax.axis_index("gx") % 2) == 0
    lane = lane_ids()
    sub = sub_ids()

    def body(h, carry):
        for c5 in range(5):
            z = h * 5 + c5
            ut, ub, vt, vb = u7[z], u0[z], v7[z], v0[z]
            e7 = UNIT * ((ut - sroll(ut, 1)) + (vt - jnp.where(lane == 0, 0.0, lroll(vt, 1))))
            up0 = jnp.where(sub == 0, 0.0, sroll(ub, 1))
            e0 = UNIT * ((ub - up0) + (vb - jnp.where(lane == 0, 0.0, lroll(vb, 1))))
            ea = jnp.where(sub < 2, sroll(e7, -3), p7[z])
            eb = jnp.where(sub < 3, sroll(e7, -5), w7[z])
            wa = jnp.where(sub < 6, p0[z], sroll(e0, 6))
            wb = jnp.where(sub < 5, w0[z], sroll(e0, 3))
            at = 2 * SUBL * c5
            xa[h, at : at + SUBL, :] = jnp.where(even, ea, wa)
            xa[h, at + SUBL : at + 2 * SUBL, :] = jnp.where(even, eb, wb)
            xb[h, at : at + SUBL, :] = jnp.where(even, wa, ea)
            xb[h, at + SUBL : at + 2 * SUBL, :] = jnp.where(even, wb, eb)
            last = ut[SUBL - 1 : SUBL, :]
            xa[h, 80 + c5 : 81 + c5, :] = last
            xb[h, 80 + c5 : 81 + c5, :] = last
        return carry

    lax.fori_loop(0, xa.shape[0], body, 0)
    east_r = r[size_x - 5 : size_x, :]
    west_r = r[0:5, :]
    ra = jnp.where(even, east_r, west_r)
    rb = jnp.where(even, west_r, east_r)
    for ref, val in ((xa, ra), (xb, rb)):
        ref[0, 85:88, :] = val[0:3]
        ref[1, 85:87, :] = val[3:5]
        ref[1, 87:88, :] = val[4:5]
        ref[2, 85:88, :] = val[0:3]
        ref[3, 85:88, :] = val[0:3]


def blend_pack(n_gx, n_gy, m, xs, band, *refs):
    u, v, p, w, r, rate = refs[:6]
    refs = refs[6:]
    we_own, sn_own = refs[0], refs[n_gx]
    we_in = refs[1:n_gx]
    sn_in = refs[n_gx + 1 : n_gx + n_gy]
    ub, vb, pb, q, ca, cb, daa, dab, dba, dbb, rows_we, corners = refs[n_gx + n_gy :]
    gx = lax.axis_index("gx")
    gy = lax.axis_index("gy")
    chunk = pl.program_id(0)
    size_x = u.shape[1]
    blocks = size_x // SUBL
    outs = (ub, vb, pb)
    for src, dst in zip((u, v, p), outs):
        dst[...] = src[...]
    lane = lane_ids()
    sub = sub_ids()

    def band_blend(pieces, row_of):
        tall_lane = lax.broadcasted_iota(jnp.int32, rows_we.shape[1:], 1)

        @pl.when(chunk == 0)
        def _():
            for fd in range(3 * band):
                g, c = divmod(fd, 4)
                val = None
                for s, piece in enumerate(pieces):
                    moved = lroll(piece[g], m * (s - c))
                    if val is None:
                        val = moved
                    else:
                        val = jnp.where(tall_lane >= m * s, moved, val)
                rows_we[fd] = val

        wts = []
        for d in range(band):
            rt = rate[row_of(d) : row_of(d) + 1, :].astype(F32)
            wts.append(jnp.maximum(rt - float(d), 0.0) / rt)

        def body(h, carry):
            for i in range(5):
                z = h * 5 + i
                for f in range(3):
                    for d in range(band):
                        at = slice(row_of(d), row_of(d) + 1)
                        val = rows_we[f * band + d, pl.ds(chunk * ZC + z, 1), :]
                        old = outs[f][z, at, :]
                        outs[f][z, at, :] = old + wts[d] * (val - old)
            return carry

        lax.fori_loop(0, ZC // 5, body, 0)

    @pl.when(gx == 0)
    def _():
        band_blend([we_own] + [we_in[s - 1] for s in range(1, n_gx)], lambda d: d)

    @pl.when(gx == n_gx - 1)
    def _():
        band_blend(
            [we_in[n_gx - 2 - s] for s in range(n_gx - 1)] + [we_own],
            lambda d: size_x - 1 - d,
        )

    per = SUBL // xs

    def side_blend(pieces, first, dist):
        wts = []
        for b in range(blocks):
            rt = rate[SUBL * b : SUBL * (b + 1), :].astype(F32)
            wts.append(jnp.maximum(rt - dist, 0.0) / rt)

        def body(h, carry):
            for z in [h * 5 + i for i in range(5)]:
                t, c = (chunk * ZC + z) // SLOT, (chunk * ZC + z) % SLOT
                shift = jnp.mod(first - band * c + LANES, LANES)
                for f in range(3):
                    for b in range(blocks):
                        val = pieces[b * per][f, t]
                        for s in range(1, per):
                            val = jnp.where(sub // xs == s, pieces[b * per + s][f, t], val)
                        val = pltpu.roll(val, shift, 1)
                        old = outs[f][z, SUBL * b : SUBL * (b + 1), :]
                        outs[f][z, SUBL * b : SUBL * (b + 1), :] = old + wts[b] * (val - old)
            return carry

        lax.fori_loop(0, ZC // 5, body, 0)

    @pl.when(gy == 0)
    def _():
        side_blend([sn_own] + [sn_in[s - 1] for s in range(1, n_gy)], 0, lane.astype(F32))

    @pl.when(gy == n_gy - 1)
    def _():
        side_blend(
            [sn_in[n_gy - 2 - s] for s in range(n_gy - 1)] + [sn_own],
            LANES - band,
            (LANES - 1 - lane).astype(F32),
        )

    def strip_of(blocks_of):
        acc = jnp.zeros((SUBL, LANES), F32)
        for b in range(blocks):
            lo = GROUP * (b + 1)
            moved = lroll(blocks_of(b), lo + DEEP)
            acc = jnp.where((lane >= lo) & (lane < lo + GROUP), moved, acc)
        return acc

    x_even = (gx % 2) == 0
    y_even = (gy % 2) == 0
    bases = [
        jnp.where(x_even, LANES - GROUP * blocks, LANES - GROUP),
        jnp.where(x_even, LANES - GROUP, LANES - GROUP * blocks),
    ]

    def body(t, carry):
        for f, src in enumerate((ub, vb, pb, w)):
            strips = []
            for c in range(10):
                z = t * 10 + c
                strip = strip_of(lambda b: src[z, SUBL * b : SUBL * (b + 1), :])
                q[0, f * ZC + z] = strip
                strips.append(strip)
            for side in range(2):
                acc = jnp.zeros((SUBL, LANES), F32)
                for c in range(10):
                    moved = pltpu.roll(strips[c], jnp.mod(bases[side] + GROUP * c, LANES), 1)
                    here = (lane >= GROUP * c) & (lane < GROUP * (c + 1))
                    acc = jnp.where(here, moved, acc)
                corners[side, f, t] = acc
        return carry

    lax.fori_loop(0, ZC // 10, body, 0)
    strip = strip_of(lambda b: r[SUBL * b : SUBL * (b + 1), :])
    q[0, 4 * ZC] = strip
    low_half = lane % GROUP < DEEP
    for side, near, diag in ((0, ca, (daa, dab)), (1, cb, (dba, dbb))):
        corners[side, 4, 0] = pltpu.roll(strip, bases[side], 1)
        corners[side, 4, 1] = corners[side, 4, 0]
        for f in range(3):
            for t in range(2):
                near[0, 2 * f + t] = corners[side, f, t]
        for way, out in enumerate(diag):
            high = y_even if way == 0 else jnp.logical_not(y_even)
            first = jnp.where(high, 0, LANES - DEEP)
            second = jnp.where(high, DEEP, 0)
            for f in range(5):
                a = pltpu.roll(corners[side, f, 0], first, 1)
                b = pltpu.roll(corners[side, f, 1], second, 1)
                out[0, f] = jnp.where(low_half, a, b)


def prepare(u, v, f_out):
    blocks = u.shape[1] // SUBL
    lane = lane_ids()
    sub = sub_ids()

    def body(i, carry):
        for z in (2 * i, 2 * i + 1):
            for b in range(blocks):
                rows = slice(SUBL * b, SUBL * (b + 1))
                uu, vv = u[z, rows, :], v[z, rows, :]
                if b == 0:
                    up = jnp.where(sub == 0, 0.0, sroll(uu, 1))
                else:
                    up = u[z, SUBL * b - 1 : SUBL * (b + 1) - 1, :]
                left = jnp.where(lane == 0, 0.0, lroll(vv, 1))
                f_out[z, rows, :] = UNIT * ((uu - up) + (vv - left))
        return carry

    lax.fori_loop(0, u.shape[0] // 2, body, 0)


def substeps(n_gx, n_gy, *refs):
    (ub_in, vb_in, pb_in, f_in, w_in) = refs[:5]
    (r, xa, xb, qa, qb, qo, ca, cb, caa, cab, cba, cbb) = refs[5:17]
    outs = refs[17:21]
    (PM, FM, WM, GM, QM, LM, SM, KM, ub, vb, u_out, v_out, w_out, p_out, WT, KEEP, sems) = refs[21:]
    levels, size_x = ub.shape[0], ub.shape[1]
    main = pl.ds(SUBL, size_x)
    loads = []
    for n, (src, dst) in enumerate(
        (
            (pb_in, PM.at[pl.ds(0, levels), pl.ds(2 * SUBL, size_x)]),
            (f_in, FM.at[pl.ds(0, levels), main]),
            (ub_in, ub),
            (w_in, WM.at[pl.ds(1, levels), main]),
            (vb_in, vb),
        )
    ):
        copy = pltpu.make_async_copy(src, dst, sems.at[n])
        copy.start()
        loads.append(copy)
    blocks = size_x // SUBL
    full = blocks + 2
    every = range(full + 1)
    gx = lax.axis_index("gx")
    gy = lax.axis_index("gy")
    x_even = (gx % 2) == 0
    y_even = (gy % 2) == 0
    is_w, is_e = gx == 0, gx == n_gx - 1
    is_s, is_n = gy == 0, gy == n_gy - 1
    lane = lane_ids()
    sub = sub_ids()
    within = lane % GROUP
    block_of = lane // GROUP
    low_half = within < DEEP
    rim_lo, rim_hi = within == DEEP - 1, within == DEEP
    zero = jnp.zeros((SUBL, LANES), F32)
    rows = [slice(SUBL * b, SUBL * (b + 1)) for b in range(full + 2)]
    COEF, RINV, STEP = 0, 1, 2

    def strip_from(mine, cw, ce, spot):
        west = pltpu.roll(cw, jnp.mod(LANES - GROUP * spot, LANES), 1)
        east = pltpu.roll(ce, jnp.mod(LANES + GROUP * (full - 1) - GROUP * spot, LANES), 1)
        got = jnp.where(block_of == 0, west, mine)
        return jnp.where(block_of == full - 1, east, got)

    def four(k, i, late):
        aa, ab, ba, bb = caa[k, i], cab[k, i], cba[k, i], cbb[k, i]
        back = jnp.where(late, LANES - DEEP, 0)
        ahead = jnp.where(late, 0, DEEP)
        pairs = []
        for sa, sb in ((aa, ab), (ba, bb)):
            south, north = jnp.where(y_even, sb, sa), jnp.where(y_even, sa, sb)
            south, north = pltpu.roll(south, back, 1), pltpu.roll(north, ahead, 1)
            pairs.append(jnp.where(low_half, south, north))
        a, b = pairs
        return jnp.where(x_even, b, a), jnp.where(x_even, a, b)

    def strip_at(k, iq, corners, spot):
        a, b = qa[k, iq], qb[k, iq]
        mine = jnp.where(low_half == y_even, b, a)
        return strip_from(mine, corners[0], corners[1], spot)

    def strip_rows(s):
        up = sroll(s, 1)
        up = jnp.where(sub == 0, lroll(up, GROUP), up)
        dn = sroll(s, -1)
        dn = jnp.where(sub == SUBL - 1, lroll(dn, -GROUP), dn)
        return up, dn

    row_first = is_w & (block_of == 1) & (sub == 0)
    row_last = is_e & (block_of == full - 2) & (sub == SUBL - 1)
    lane0, lane_end = lane == 0, lane == LANES - 1
    lane0_in = lane0 & jnp.logical_not(is_s)
    strip_zero = is_n & rim_hi
    fix_w, fix_e = is_w & (sub == SUBL - 1), is_e & (sub == 0)

    def put_pressure(z, tiles):
        tiles = list(tiles)
        tiles[0] = jnp.where(fix_w, sroll(tiles[1], -1), tiles[0])
        tiles[full - 1] = jnp.where(fix_e, 0.0, tiles[full - 1])
        ps = jnp.where(strip_zero, 0.0, tiles[full])
        PM[z, rows[full + 1], :] = ps
        for b in range(full):
            PM[z, rows[b + 1], :] = tiles[b]
        up, dn = strip_rows(ps)
        up = jnp.where(row_first, ps, up)
        dn = jnp.where(row_last, 0.0, dn)
        LM[z] = up + dn

    k_id = lax.broadcasted_iota(jnp.int32, (LANES, LANES), 0)
    l_id = lax.broadcasted_iota(jnp.int32, (LANES, LANES), 1)
    beside = (k_id == l_id + 1) | (k_id == l_id - 1)
    beside = beside | (is_s & (k_id == 0) & (l_id == 0))
    rim = ((l_id % GROUP == DEEP - 1) & (k_id == LANES - 1)) | (
        (l_id % GROUP == DEEP) & (k_id == 0)
    )
    fill = ((k_id % GROUP == DEEP - 1) & (l_id == 0) & jnp.logical_not(is_s)) | (
        (k_id % GROUP == DEEP) & (l_id == LANES - 1)
    )
    for part in range(2):
        at = 2 * LANES * part
        WT[at : at + LANES, 0:LANES] = beside.astype(F32).astype(BF16)
        WT[at : at + LANES, LANES:] = rim.astype(F32).astype(BF16)
        WT[at + LANES : at + 2 * LANES, 0:LANES] = fill.astype(F32).astype(BF16)
        WT[at + LANES : at + 2 * LANES, LANES:] = jnp.zeros((LANES, LANES), BF16)
    for b in range(full):
        KEEP[rows[b], :] = (block_of == b).astype(F32)

    def halves(x):
        high = x.astype(BF16)
        return high, (x - high.astype(F32)).astype(BF16)

    west_x = lambda h, lo, hi: jnp.where(x_even, xb[h, lo:hi, :], xa[h, lo:hi, :])
    east_x = lambda h, lo, hi: jnp.where(x_even, xa[h, lo:hi, :], xb[h, lo:hi, :])
    KM[COEF] = jnp.ones(KM.shape[1:], F32)
    KM[COEF, SUBL : SUBL * (blocks + 1), :] = r[...]
    KM[COEF, 3:6, :] = west_x(0, 85, 88)
    KM[COEF, 6:8, :] = west_x(1, 85, 87)
    lo = SUBL * (full - 1)
    KM[COEF, lo : lo + 3, :] = east_x(0, 85, 88)
    KM[COEF, lo + 3 : lo + 5, :] = east_x(1, 85, 87)
    KM[COEF, rows[full], :] = strip_at(0, 4 * ZC, four(0, 4, False), 0)
    kappas, rhos = [], []
    for b in every:
        c = KM[COEF, rows[b], :]
        c = jnp.where(c > 0.0, c, 1.0)
        KM[RINV, rows[b], :] = 1.0 / c
        KM[STEP, rows[b], :] = BUOYANCY / c
        k = 2.0 * c / ((1.0 + 2.0 * c) + jnp.sqrt(1.0 + 4.0 * c))
        kappas.append(k)
        rhos.append(k * k)

    def factor_body(z, carry):
        powers, lows = [], []
        for b in every:
            powers.append(carry[0][b] * rhos[b])
            lows.append(1.0 - powers[b])
            GM[z + 1, rows[b], :] = kappas[b] * (carry[1][b] / lows[b])
        return tuple(powers), tuple(lows)

    lax.fori_loop(0, levels, factor_body, (tuple(rhos), tuple(1.0 - x for x in rhos)))
    wide = jnp.zeros(FM.shape[1:], F32)
    GM[0] = wide
    WM[0] = wide
    for z in range(levels, FM.shape[0]):
        FM[z] = wide
        LM[z] = zero
        PM[z] = wide
        SM[z] = wide

    s5 = ZC // 5

    def patch(near, side, spot, p_old, f_old):
        shift = jnp.mod(LANES - GROUP * spot - DEEP, LANES)
        uu, vv, pp = [pltpu.roll(near[f][side], shift, 1) for f in range(3)]
        up = sroll(uu, 1)
        if side == 1:
            up = jnp.where(sub == 0, 0.0, up)
        f_new = UNIT * ((uu - up) + (vv - jnp.where(lane0, 0.0, lroll(vv, 1))))
        mine_s, mine_n = is_s & (lane < DEEP), is_n & (lane > LANES - DEEP)
        here = mine_s | mine_n
        return jnp.where(here, pp, p_old), jnp.where(here, f_new, f_old), (here, uu)

    def unpack(patched, h, carry):
        k, hh = h // s5, h % s5
        late = hh // 2
        corners = [four(k, f, late == 1) for f in range(4)]
        near = []
        for f in range(3):
            a, b = ca[k, 2 * f + late], cb[k, 2 * f + late]
            near.append((jnp.where(x_even, b, a), jnp.where(x_even, a, b)))
        v_w, v_e = near[1]
        for c5 in range(5):
            z, zz = h * 5 + c5, hh * 5 + c5
            spot = (hh % 2) * 5 + c5
            us, vs, ps, ws = [strip_at(k, f * ZC + zz, corners[f], spot) for f in range(4)]
            at = 2 * SUBL * c5
            xa_a, xa_b = xa[h, at : at + SUBL, :], xa[h, at + SUBL : at + 2 * SUBL, :]
            xb_a, xb_b = xb[h, at : at + SUBL, :], xb[h, at + SUBL : at + 2 * SUBL, :]
            wa, wb = jnp.where(x_even, xb_a, xa_a), jnp.where(x_even, xb_b, xa_b)
            ea, eb = jnp.where(x_even, xa_a, xb_a), jnp.where(x_even, xa_b, xb_b)
            f_west = jnp.where(sub < 5, sroll(wa, 3), sroll(wb, 5))
            f_east = jnp.where(sub < 2, sroll(ea, 2), sroll(eb, -3))
            u_side = None
            if patched:
                wa, f_west, u_side = patch(near, 0, spot, wa, f_west)
                ea, f_east, _ = patch(near, 1, spot, ea, f_east)
            u_row = jnp.where(x_even, xb[h, 80 + c5 : 81 + c5, :], xa[h, 80 + c5 : 81 + c5, :])
            if u_side is not None:
                here, uu = u_side
                u_row = jnp.where(here, sroll(uu, 1), u_row)
            u_row = jnp.where(is_w, 0.0, u_row)
            v_left = jnp.where(block_of == 0, zero, qo[k, ZC + zz])
            far = strip_from(v_left, v_w, v_e, spot)
            v_left = lroll(jnp.where(rim_lo, far, vs), 1)
            u_up, _ = strip_rows(us)
            FM[z, rows[full], :] = UNIT * ((us - u_up) + (vs - v_left))
            WM[z + 1, rows[full], :] = ws
            WM[z + 1, rows[0], :] = wb
            WM[z + 1, rows[full - 1], :] = eb
            ps = jnp.where(strip_zero, 0.0, ps)
            wa = jnp.where(fix_w, sroll(PM[z, rows[2], :], -1), wa)
            ea = jnp.where(fix_e, 0.0, ea)
            PM[z, rows[0], :] = zero
            PM[z, rows[1], :] = wa
            PM[z, rows[full], :] = ea
            PM[z, rows[full + 1], :] = ps
            up, dn = strip_rows(ps)
            up = jnp.where(row_first, ps, up)
            dn = jnp.where(row_last, 0.0, dn)
            LM[z] = up + dn
            for b in range(full):
                lo = GROUP * b + DEEP
                less = jnp.where(lane0, lroll(vs, 1 - lo), 0.0)
                if b == 0:
                    f = f_west
                elif b == full - 1:
                    f = f_east
                    u63 = sroll(ub[z, rows[blocks - 1], :], 1)
                    less = less + jnp.where(sub == 0, u63, 0.0)
                else:
                    f = FM[z, rows[b], :]
                    if b == 1:
                        less = less + jnp.where(sub == 0, u_row, 0.0)
                FM[z, rows[b], :] = f - UNIT * less
            SM[z] = wide
        return carry

    rim = is_s | is_n
    for copy in loads[:3]:
        copy.wait()

    @pl.when(rim)
    def _():
        lax.fori_loop(0, levels // 5, functools.partial(unpack, True), 0)

    @pl.when(jnp.logical_not(rim))
    def _():
        lax.fori_loop(0, levels // 5, functools.partial(unpack, False), 0)

    coef_step = ACCEL * SPREAD
    inner = range(1, full - 1)

    def sections(levels_of, last):
        mask = KEEP[...]
        parts = []
        for z in levels_of:
            p_high, p_low = halves(PM[z, SUBL : SUBL * (full + 1), :])
            s_high, s_low = halves(
                jnp.concatenate([PM[z, rows[full + 1], :]] * full, axis=0) * mask
            )
            parts.append(jnp.concatenate([p_high, s_high, p_low, s_low], axis=1))
        moved = jnp.dot(
            jnp.concatenate(parts, axis=0), WT[...], preferred_element_type=F32
        )
        tall = SUBL * full
        for n, z in enumerate(levels_of):
            section(z, moved[tall * n : tall * (n + 1)], last)

    def section(z, moved, last):
        ps = PM[z, rows[full + 1], :]
        rims = zero
        for b in every:
            p0 = PM[z, rows[b + 1], :]
            if b >= 1:
                SM[z, rows[b - 1], :] += p0
            if last and b not in inner:
                continue
            if b < full:
                rims = jnp.where(block_of == b, moved[rows[b], LANES:], rims)
                up = PM[z, SUBL * (b + 1) - 1 : SUBL * (b + 2) - 1, :]
                dn = PM[z, SUBL * (b + 1) + 1 : SUBL * (b + 2) + 1, :]
                around = moved[rows[b], 0:LANES] + (up + dn)
            else:
                s_lf = lroll(jnp.where(rim_lo, rims, ps), 1)
                s_rt = lroll(jnp.where(rim_hi, rims, ps), -1)
                around = LM[z] + (s_lf + s_rt)
            f = FM[z, rows[b], :] + (4.0 * p0 - around)
            if not last:
                FM[z, rows[b], :] = f
            QM[z, rows[b], :] = p0 - coef_step * f

    def run_step(last):
        active = inner if last else every
        sections(range(FORE + 1), last)

        def forward(i, carry):
            d_prev = dict(zip(active, carry))
            sections([FORE * i + FORE + 1 + c for c in range(FORE)], last)
            q_here = {b: QM[FORE * i, rows[b], :] for b in active}
            for c in range(FORE):
                z = FORE * i + c
                for b in active:
                    q_next = QM[z + 1, rows[b], :]
                    change = q_here[b] - q_next
                    q_here[b] = q_next
                    rhs = WM[z + 1, rows[b], :] * KM[RINV, rows[b], :] + KM[STEP, rows[b], :] * change
                    d = GM[z + 1, rows[b], :] * (rhs + d_prev[b])
                    WM[z + 1, rows[b], :] = d
                    d_prev[b] = d
            return tuple(d_prev[b] for b in active)

        tops = lax.fori_loop(0, levels // FORE, forward, tuple(zero for _ in active))

        def backward(i, above):
            above = dict(zip(active, above))
            for c in range(BACK):
                z = levels - 1 - (BACK * i + c)
                tiles = {}
                below = {}
                for b in active:
                    ww = WM[z, rows[b], :] + GM[z, rows[b], :] * above[b]
                    tiles[b] = QM[z, rows[b], :] - BUOYANCY * (above[b] - ww)
                    if not last:
                        WM[z, rows[b], :] = ww
                    below[b] = ww
                if last:
                    ss = SM[z, rows[blocks + 1], :]
                    for b in active:
                        m = rows[b - 1]
                        w_out[z, m, :] = above[b]
                        p_out[z, m, :] = tiles[b]
                        s0 = SM[z, m, :]
                        dn = SM[z, SUBL * (b - 1) + 1 : SUBL * b + 1, :]
                        rt = jnp.where(
                            lane_end, lroll(ss, -1 - (GROUP * b + DEEP)), lroll(s0, -1)
                        )
                        u_out[z, m, :] = ub[z, m, :] - ACCEL * (dn - s0)
                        v_out[z, m, :] = vb[z, m, :] - ACCEL * (rt - s0)
                else:
                    put_pressure(z, [tiles[b] for b in every])
                above = below
            if last:
                part = pl.ds(levels - BACK - BACK * i, BACK)
                for n, (src, dst) in enumerate(zip((u_out, v_out, w_out, p_out), outs)):
                    pltpu.make_async_copy(src.at[part], dst.at[part], sems.at[5 + n]).start()
            return tuple(above[b] for b in active)

        lax.fori_loop(0, levels // BACK, backward, tops)

    loads[3].wait()

    def step(_, carry):
        run_step(False)
        return carry

    lax.fori_loop(0, SUBSTEPS - 1, step, 0)
    loads[4].wait()
    run_step(True)
    for n, (src, dst) in enumerate(zip((u_out, v_out, w_out, p_out), outs)):
        pltpu.make_async_copy(src, dst, sems.at[5 + n]).wait()


def swap(block, axis, second):
    n = lax.axis_size(axis)
    return lax.ppermute(block, axis, pairing(n, second))


def pairing(n, second):
    lo = 1 if second else 0
    pairs = []
    for i in range(lo, n - 1, 2):
        pairs += [(i, i + 1), (i + 1, i)]
    return pairs


def swap2(block, second_x, second_y):
    nx, ny = lax.axis_size("gx"), lax.axis_size("gy")
    pairs = []
    for a, b in pairing(nx, second_x):
        for c, d in pairing(ny, second_y):
            pairs.append((a * ny + c, b * ny + d))
    return lax.ppermute(block, ("gx", "gy"), pairs)


def to_ends(own, blocks, axis):
    n = lax.axis_size(axis)
    got = [own]
    for k, block in enumerate(blocks, 1):
        got.append(lax.ppermute(block, axis, [(k, 0), (n - 1 - k, n - 1)]))
    return got


def per_device(u_wind, v_wind, w_wind, pressure, vert_coef, we_slab, sn_slab, relax_width):
    n_gx, n_gy = lax.axis_size("gx"), lax.axis_size("gy")
    levels, size_x, size_y = pressure.shape
    blocks = size_x // SUBL
    full = blocks + 2
    band, m = we_slab.shape[3], we_slab.shape[4]
    xs = sn_slab.shape[4]
    steps = levels // ZC
    sds = jax.ShapeDtypeStruct
    big = pltpu.CompilerParams(vmem_limit_bytes=60 * 1024 * 1024)
    vmem = pl.BlockSpec(memory_space=pltpu.VMEM)

    lead = lambda shape: pl.BlockSpec((1,) + shape[1:], lambda i: (i,) + (0,) * (len(shape) - 1))
    fixed = lambda shape: pl.BlockSpec(shape, lambda i: (0,) * len(shape))
    field = pl.BlockSpec((ZC, size_x, size_y), lambda i: (i, 0, 0))
    low = pl.BlockSpec((ZC, SUBL, size_y), lambda i: (i, 0, 0))
    high = pl.BlockSpec((ZC, SUBL, size_y), lambda i: (i, blocks - 1, 0))
    plane = pl.BlockSpec((size_x, size_y), lambda i: (0, 0))
    x_shape = (levels // 5, 88, LANES)
    rows_call = pl.pallas_call(
        functools.partial(pack_rows, size_x),
        grid=(steps,),
        in_specs=[low, high] * 4 + [plane],
        out_specs=[pl.BlockSpec((ZC // 5, 88, LANES), lambda i: (i, 0, 0))] * 2,
        out_shape=[sds(x_shape, F32)] * 2,
        name="pack_rows",
    )
    xa, xb = rows_call(
        u_wind, u_wind, v_wind, v_wind, pressure, pressure, w_wind, w_wind, vert_coef,
    )
    xa = swap(xa, "gx", False)
    xb = swap(xb, "gx", True)

    we_t = jnp.transpose(we_slab, (0, 1, 3, 4, 2))
    sn_t = jnp.transpose(sn_slab, (0, 1, 3, 4, 2))
    we_shape = (-(-3 * band // 4), 64, LANES)
    sn_shape = (3, -(-levels // SLOT), SUBL, LANES)
    pack_call = pl.pallas_call(
        functools.partial(pack_slabs, n_gx, n_gy),
        in_specs=[vmem] * 2,
        out_specs=[vmem] * (n_gx + n_gy),
        out_shape=[sds(we_shape, F32)] * n_gx + [sds(sn_shape, F32)] * n_gy,
        scratch_shapes=[
            pltpu.VMEM((2, LANES, LANES), F32),
            pltpu.VMEM((2, band, 3 * SUBL, LANES), F32),
        ],
        name="pack_slabs",
    )
    packed = pack_call(we_t, sn_t)
    we_all = to_ends(packed[0], packed[1:n_gx], "gx")
    sn_all = to_ends(packed[n_gx], packed[n_gx + 1 :], "gy")

    q_shape = (steps, 4 * ZC + 4, SUBL, LANES)
    c_shape = (steps, 6, SUBL, LANES)
    d_shape = (steps, 5, SUBL, LANES)
    blend_call = pl.pallas_call(
        functools.partial(blend_pack, n_gx, n_gy, m, xs, band),
        grid=(steps,),
        in_specs=[field] * 4
        + [plane] * 2
        + [fixed(we_shape)] * n_gx
        + [fixed(sn_shape)] * n_gy,
        out_specs=[field] * 3 + [lead(q_shape)] + [lead(c_shape)] * 2 + [lead(d_shape)] * 4,
        out_shape=[sds(pressure.shape, F32)] * 3
        + [sds(q_shape, F32)]
        + [sds(c_shape, F32)] * 2
        + [sds(d_shape, F32)] * 4,
        scratch_shapes=[
            pltpu.VMEM((3 * band, 64, LANES), F32),
            pltpu.VMEM((2, 5, 2, SUBL, LANES), F32),
        ],
        compiler_params=big,
        name="blend_pack",
    )
    ub, vb, pb, q, ca, cb, caa, cab, cba, cbb = blend_call(
        u_wind, v_wind, pressure, w_wind, vert_coef, relax_width, *we_all, *sn_all
    )
    qa = swap(q, "gy", False)
    qb = swap(q, "gy", True)
    ca = swap(ca, "gx", False)
    cb = swap(cb, "gx", True)
    caa = swap2(caa, False, False)
    cab = swap2(cab, False, True)
    cba = swap2(cba, True, False)
    cbb = swap2(cbb, True, True)
    prep_call = pl.pallas_call(
        prepare,
        grid=(steps,),
        in_specs=[field] * 2,
        out_specs=field,
        out_shape=sds(pressure.shape, F32),
        compiler_params=big,
        name="prepare",
    )
    f_main = prep_call(ub, vb)

    whole = pl.BlockSpec(memory_space=pltpu.VMEM)
    tall = pltpu.VMEM((levels + FORE + 1, 96, LANES), F32)
    own = pltpu.VMEM(pressure.shape, F32)
    far = pl.BlockSpec(memory_space=pl.ANY)
    return pl.pallas_call(
        functools.partial(substeps, n_gx, n_gy),
        in_specs=[far] * 5 + [whole] * 12,
        out_specs=[far] * 4,
        out_shape=[sds(pressure.shape, F32)] * 4,
        scratch_shapes=[tall] * 5
        + [pltpu.VMEM((levels + FORE + 1, SUBL, LANES), F32), tall]
        + [pltpu.VMEM((3, 96, LANES), F32)]
        + [own] * 6
        + [pltpu.VMEM((4 * LANES, 2 * LANES), BF16), pltpu.VMEM((SUBL * full, LANES), F32)]
        + [pltpu.SemaphoreType.DMA((9,))],
        compiler_params=big,
        name="substeps",
    )(
        ub, vb, pb, f_main, w_wind,
        vert_coef, xa, xb, qa, qb, q, ca, cb, caa, cab, cba, cbb,
    )


def solution(mesh):
    cell = P(None, "gx", "gy")
    placed = (
        cell, cell, cell, cell,
        P("gx", "gy"),
        P(None, None, None, None, ("gy", "gx")),
        P(None, None, None, None, ("gx", "gy")),
        P("gx", "gy"),
    )
    return jax.shard_map(
        per_device,
        mesh=mesh,
        in_specs=placed,
        out_specs=(cell, cell, cell, cell),
        check_vma=False,
    )
```
